256 devices in a mesh: blk: 256 (over y, z, x, core).
Axes of the slice: x: 4, y: 4, z: 8, core: 2. Of those that a mesh axis runs over, the one named last changes fastest.
Arguments:
- image_features: bfloat16 [65536, 1536], P('blk'), may hold values from -0.5 to 0.5
- head_weight: bfloat16 [1536, 1152], P('blk'), may hold values from -0.15625 to 0.15625
- text_embeds: bfloat16 [65536, 1152], P('blk'), may hold values from -0.29882812 to 0.29882812
- natural_exponent_factor: float32 [1], replicated, may hold values from 1.6 to 2.6
- logit_bias: float32 [1], replicated, may hold values from -4 to -1
Outputs:
- grad_features: bfloat16 [65536, 1536], P('blk')
- grad_text: bfloat16 [65536, 1152], P('blk')
- grad_weight: float32 [1536, 1152], P('blk')
The draws below stay inside these ranges and needn't reach their ends.
All inputs are finite; a program needn't handle non-finite values.
Results may differ from the reference program's by a relative error of at most 0.0085.
Values may be sent and summed in bfloat16 or wider, within the bound.
No kernel may reach another device: no remote copies, remote signals or barrier semaphores. Data moves between devices by JAX's collectives and lax.ppermute only.
A program may use at most 64 MiB of HBM per device.

```python
import jax
import jax.numpy as jnp
from jax import lax

D = 1536
E = 1152
R = 256
S = 4
TOTAL = 65536
N_BLK = 256


def strengthened(entries, rng, source, target, blocks, factor):
    owner, partner = [(jnp.arange(entries.shape[axis_at]) // (entries.shape[axis_at] // blocks)).reshape([-1 if axis == axis_at else 1 for axis in range(entries.ndim)]) for axis_at in (source, target)]
    chosen = jax.random.permutation(rng, blocks)[partner]
    strong = (owner == chosen) | (owner == (partner + blocks // 2) % blocks)
    return jnp.where(strong, factor * entries, entries)


def levels(rng, extent, split, least, largest):
    def one(position, parts):
        steps = jax.random.uniform(jax.random.fold_in(jax.random.fold_in(rng, 6), position), (parts,), jnp.float32, least / len(split), largest / len(split))
        return jnp.repeat(jnp.exp(steps), extent[position] // parts).reshape((-1,) + (1,) * (len(extent) - position - 1))

    level = one(*split[0])
    for cut in split[1:]:
        level = level * one(*cut)
    return level


def bell_draw(stream_key, dims, scale, bound, pieces=(), kind=jnp.bfloat16):
    drawn = jax.random.normal(stream_key, dims, jnp.float32) * scale
    if len(pieces) > 0:
        drawn = levels(stream_key, dims, pieces, -0.22, 0.18) * drawn
    return jnp.clip(drawn, min=-bound, max=bound).astype(kind)


def heavy_noise(key, shape, spread, reach, pieces, heavy, kind=jnp.bfloat16):
    drawn = spread * jax.random.normal(key, shape, jnp.float32)
    if pieces:
        drawn = drawn * levels(key, shape, pieces, -0.22, 0.18)
    return jnp.clip(strengthened(drawn, jax.random.fold_in(key, 3), *heavy), -reach, reach).astype(kind)


def setup_inputs(seed: int = 0) -> dict:
    streams_of = jax.random.split(jax.random.key(seed), 6)
    return {
        "image_features": heavy_noise(streams_of[0], (TOTAL, D), 0.02, 0.5, ((0, 256),), (0, 1, 256, 6.0)),
        "head_weight": bell_draw(streams_of[1], (D, E), D ** -0.5, 0.15625, ((0, 256),)),
        "text_embeds": bell_draw(streams_of[2], (TOTAL, E), 0.05, 0.29882812, ((0, 256),)),
        "natural_exponent_factor": jnp.clip(jax.random.uniform(streams_of[3], (1,), jnp.float32, 1.6, 2.6), 1.6, 2.6),
        "logit_bias": jnp.clip(jax.random.uniform(streams_of[4], (1,), jnp.float32, -4.0, -1.0), -4.0, -1.0),
    }


epsilon = 1e-06

def normalize(rows):
    squares = lax.optimization_barrier(jnp.sum(rows * rows, axis=1, keepdims=True))
    length = jnp.sqrt(squares + epsilon)
    return (rows / length, length)

def similarity_derivative(picture_sample_group, caption_sample_group, similarity_multiplier, neighbour_distance, outer_dimension_size):
    similarity_matrix = similarity_multiplier * lax.dot_general(picture_sample_group, caption_sample_group, (((1,), (1,)), ((), ())), preferred_element_type=jnp.float32) + neighbour_distance
    if outer_dimension_size:
        matched = lax.broadcasted_iota(jnp.int32, similarity_matrix.shape, 0) == lax.broadcasted_iota(jnp.int32, similarity_matrix.shape, 1)
        match_polarity = jnp.where(matched, 1.0, -1.0).astype(jnp.float32)
    else:
        match_polarity = -jnp.ones(similarity_matrix.shape, jnp.float32)
    return (-similarity_multiplier * match_polarity * jax.nn.sigmoid(-match_polarity * similarity_matrix)).astype(jnp.bfloat16)

def project_back(grad, unit_rows, length):
    return (grad - unit_rows * lax.optimization_barrier(jnp.sum(unit_rows * grad, axis=1, keepdims=True))) / length

def reference(image_features, head_weight, text_embeds, natural_exponent_factor, logit_bias):
    embedded = jnp.dot(image_features, head_weight, preferred_element_type=jnp.float32)
    image_unit, image_length = normalize(embedded)
    picture_embedding_mapped = image_unit.astype(jnp.bfloat16)
    text_unit, text_length = normalize(text_embeds.astype(jnp.float32))
    text_low = text_unit.astype(jnp.bfloat16)
    similarity_multiplier = jnp.exp(natural_exponent_factor[0])
    neighbour_distance = logit_bias[0]
    image_blocks = picture_embedding_mapped.reshape(N_BLK, R, E)
    text_blocks = text_low.reshape(N_BLK, R, E)

    def pick_block(blocks, block_id):
        where_at = ((block_id + N_BLK) % N_BLK).astype(jnp.int32)
        return lax.dynamic_index_in_dim(blocks, where_at, 0, keepdims=False)

    def image_side(block_id):
        picture_sample_group = pick_block(image_blocks, block_id)
        summed = jnp.zeros((R, E), jnp.float32)
        for partition_portion in range(S):
            caption_sample_group = pick_block(text_blocks, block_id + partition_portion)
            mapping_matrix = similarity_derivative(picture_sample_group, caption_sample_group, similarity_multiplier, neighbour_distance, partition_portion == 0)
            summed = summed + jnp.dot(mapping_matrix, caption_sample_group, preferred_element_type=jnp.float32)
        return summed

    def text_side(block_id):
        caption_sample_group = pick_block(text_blocks, block_id)
        summed = jnp.zeros((R, E), jnp.float32)
        for partition_portion in range(S):
            picture_sample_group = pick_block(image_blocks, block_id - partition_portion)
            mapping_matrix = similarity_derivative(picture_sample_group, caption_sample_group, similarity_multiplier, neighbour_distance, partition_portion == 0)
            summed = summed + lax.dot_general(mapping_matrix, picture_sample_group, (((0,), (0,)), ((), ())), preferred_element_type=jnp.float32)
        return summed
    block_ids = jnp.arange(N_BLK, dtype=jnp.int32)
    image_grad = lax.map(image_side, block_ids).reshape(-1, E)
    text_grad = lax.map(text_side, block_ids).reshape(-1, E)
    embed_grad = project_back(image_grad, image_unit, image_length).astype(jnp.bfloat16)
    grad_text = project_back(text_grad, text_unit, text_length).astype(jnp.bfloat16)
    grad_features = lax.dot_general(embed_grad, head_weight, (((1,), (1,)), ((), ())), preferred_element_type=jnp.float32).astype(jnp.bfloat16)
    grad_weight = lax.dot_general(image_features, embed_grad, (((0,), (0,)), ((), ())), preferred_element_type=jnp.float32)
    return (grad_features, grad_text, grad_weight)
```

```python
import functools

import jax
import jax.numpy as jnp
from jax import lax
from jax.experimental import pallas as pl
from jax.experimental.pallas import tpu as pltpu
from jax.sharding import Mesh
from jax.sharding import PartitionSpec as P


S = 4
EPS = 1e-06
NY, NZ, NX, NC = 4, 8, 4, 2
NDEV = NY * NZ * NX * NC
AXES = ("y", "z", "x", "c")
R, D, E = 256, 1536, 1152
HALF = D // 2
PIECE = HALF // 4
SUB = PIECE // 4
OWN = D // NDEV
F32, BF16 = jnp.float32, jnp.bfloat16
NN = (((1,), (0,)), ((), ()))
NT = (((1,), (1,)), ((), ()))
COLS = 384


def mm(a, b, dims=NN):
    return lax.dot_general(a, b, dims, preferred_element_type=F32)


def index(y, z, x, c):
    return ((y % NY * NZ + z % NZ) * NX + x % NX) * NC + c % NC


def coords(i):
    return i // (NZ * NX * NC), i // (NX * NC) % NZ, i // NC % NX, i % NC


def fetch(value, where):
    return lax.ppermute(value, AXES, [(index(*where(*coords(i))), i) for i in range(NDEV)])


def along_z(d):
    return lambda y, z, x, c: (y, z + d, x, c)


def along_first(d):
    return lambda y, z, x, c: (y, z, x + d, c) if c == 0 else (y + d, z, x, c)


def along_second(d):
    return lambda y, z, x, c: (y + d, z, x, c) if c == 0 else (y, z, x + d, c)


def sibling(y, z, x, c):
    return y, z, x, 1 - c


def along_blocks(d):
    return lambda y, z, x, c: coords((index(y, z, x, c) + d) % NDEV)


def call(body, outs, *args, flops=0, scratch=(), smem=()):
    def spec(i):
        return pl.BlockSpec(memory_space=pltpu.SMEM if i in smem else pltpu.VMEM)

    return pl.pallas_call(
        body,
        out_shape=[jax.ShapeDtypeStruct(s, d) for s, d in outs],
        in_specs=[spec(i) for i in range(len(args))],
        out_specs=[pl.BlockSpec(memory_space=pltpu.VMEM) for _ in outs],
        scratch_shapes=list(scratch),
        cost_estimate=pl.CostEstimate(flops=flops, bytes_accessed=0, transcendentals=0),
    )(*args)


def text_body(raw_ref, low_ref, length_ref):
    raw = raw_ref[...].astype(F32)
    length = jnp.sqrt(jnp.sum(raw * raw, axis=1, keepdims=True) + EPS)
    length_ref[...] = length
    low_ref[...] = (raw / length).astype(BF16)


def order_body(source_ref, x_ref, pick_ref, xp_ref, xpt_ref):
    step = 256
    for at in range(0, D, step):
        rows = pl.ds(at, step)
        lanes = lax.broadcasted_iota(jnp.int32, (step, D), 1)
        pick = jnp.where(lanes == source_ref[rows, :], 1.0, 0.0).astype(BF16)
        pick_ref[rows, :] = pick
        xpt_ref[rows, :] = mm(pick, x_ref[...], NT).astype(BF16)
        xp_ref[:, rows] = mm(x_ref[...], pick, NT).astype(BF16)


def embed_body(xp_ref, *refs):
    pieces, (w_ref, unit_ref, low_ref, length_ref) = refs[:8], refs[8:]
    for i, piece in enumerate(pieces):
        w_ref[pl.ds(i * PIECE, PIECE), :] = piece[...]
    squares = jnp.zeros((R, 1), F32)
    for at in range(0, E, COLS):
        cols = pl.ds(at, COLS)
        part = mm(xp_ref[...], w_ref[:, cols])
        unit_ref[:, cols] = part
        squares = squares + jnp.sum(part * part, axis=1, keepdims=True)
    length = jnp.sqrt(squares + EPS)
    length_ref[...] = length
    unit = unit_ref[...] / length
    unit_ref[...] = unit
    low_ref[...] = unit.astype(BF16)


def derivative(rows, columns, scale, bias, diagonal):
    logits = scale * mm(rows, columns, NT) + bias
    if not diagonal:
        return (scale * jax.nn.sigmoid(logits)).astype(BF16)
    matched = lax.broadcasted_iota(jnp.int32, logits.shape, 0) == lax.broadcasted_iota(
        jnp.int32, logits.shape, 1
    )
    polarity = jnp.where(matched, 1.0, -1.0)
    return (-scale * polarity * jax.nn.sigmoid(-polarity * logits)).astype(BF16)


def image_body(scalar_ref, low_ref, unit_ref, length_ref, t0, t1, t2, t3, xpt_ref, eg_ref, gw_ref, grad, pair):
    scale, bias = scalar_ref[0], scalar_ref[1]
    texts = (t0, t1, t2, t3)
    for k, text in enumerate(texts):
        pair[k] = derivative(low_ref[...], text[...], scale, bias, k == 0)
    inner = jnp.zeros((R, 1), F32)
    for at in range(0, E, COLS):
        cols = pl.ds(at, COLS)
        part = mm(pair[0], t0[:, cols])
        for k in range(1, S):
            part = part + mm(pair[k], texts[k][:, cols])
        grad[:, cols] = part
        inner = inner + jnp.sum(part * unit_ref[:, cols], axis=1, keepdims=True)
    eg_ref[...] = ((grad[...] - unit_ref[...] * inner) / length_ref[...]).astype(BF16)
    for at in range(0, HALF, PIECE):
        rows = pl.ds(at, PIECE)
        gw_ref[rows, :] = mm(xpt_ref[pl.ds(HALF + at, PIECE), :], eg_ref[...]).astype(BF16)


def weight_body(xpt_ref, eg_ref, came_ref, *outs):
    for i, out in enumerate(outs):
        rows = pl.ds(i * PIECE, PIECE)
        out[...] = (mm(xpt_ref[rows, :], eg_ref[...]) + came_ref[rows, :].astype(F32)).astype(BF16)


def features_body(eg_ref, w_ref, pick_ref, out_ref, mixed):
    for at in range(0, D, COLS):
        rows = pl.ds(at, COLS)
        mixed[:, rows] = mm(eg_ref[...], w_ref[rows, :], NT).astype(BF16)
    for at in range(0, D, COLS):
        cols = pl.ds(at, COLS)
        out_ref[:, cols] = mm(mixed[...], pick_ref[:, cols]).astype(BF16)


def text_grad_body(scalar_ref, raw_ref, low_ref, length_ref, p0, p1, p2, p3, out_ref, grad, pair):
    scale, bias = scalar_ref[0], scalar_ref[1]
    images = (p0, p1, p2, p3)
    for k, image in enumerate(images):
        pair[k] = derivative(low_ref[...], image[...], scale, bias, k == 0)
    length = length_ref[...]
    inner = jnp.zeros((R, 1), F32)
    for at in range(0, E, COLS):
        cols = pl.ds(at, COLS)
        part = mm(pair[0], p0[:, cols])
        for k in range(1, S):
            part = part + mm(pair[k], images[k][:, cols])
        grad[:, cols] = part
        inner = inner + jnp.sum(part * (raw_ref[:, cols].astype(F32) / length), axis=1, keepdims=True)
    out_ref[...] = ((grad[...] - raw_ref[...].astype(F32) / length * inner) / length).astype(BF16)


def sum_body(*refs, cuts):
    ins, outs = refs[:4], refs[4:]
    total = ins[0][...].astype(F32)
    for ref in ins[1:]:
        total = total + ref[...].astype(F32)
    for out, (lo, hi) in zip(outs, cuts, strict=True):
        out[...] = total[lo:hi].astype(BF16)


def near_body(mid_ref, low_ref, high_ref, *outs):
    mid, low, high = (ref[...].astype(F32) for ref in (mid_ref, low_ref, high_ref))
    outs[0][...] = (mid[:OWN] + low[:OWN] + high[:OWN]).astype(BF16)
    outs[1][...] = mid[OWN : 2 * OWN] + low[OWN:] + high[OWN : 2 * OWN]
    outs[2][...] = (mid[2 * OWN :] + high[2 * OWN :]).astype(BF16)


def row_sources():
    y, z, x, c = (lax.axis_index(a) for a in AXES)
    k = lax.broadcasted_iota(jnp.int32, (D, 1), 0)
    core = jnp.where(k < HALF, c, 1 - c)
    k = k % HALF
    second, first, near, row = k // PIECE, k % PIECE // SUB, k % SUB // OWN, k % OWN
    at_y = (y + jnp.where(core == 0, second, first)) % NY
    at_x = (x + jnp.where(core == 0, first, second)) % NX
    at_z = (z + near + (NZ - 3)) % NZ
    return (((at_y * NZ + at_z) * NX + at_x) * NC + core) * OWN + row


def gather_weight(w):
    near = jnp.concatenate([fetch(w, along_z(-1)), w, fetch(w, along_z(1))], 0)
    high, low = fetch(near, along_z(3)), fetch(near, along_z(-2))
    ring = jnp.concatenate([low[: 2 * OWN], near, high], 0)
    plane = jnp.concatenate([ring] + [fetch(ring, along_first(d)) for d in (1, 2, 3)], 0)
    half = [plane] + [fetch(plane, along_second(d)) for d in (1, 2, 3)]
    return half + [fetch(piece, sibling) for piece in half]


def scatter_weight(pieces):
    got = [pieces[0]] + [fetch(pieces[d], along_second(-d)) for d in (1, 2, 3)]
    cuts = [(i * SUB, (i + 1) * SUB) for i in range(4)]
    pieces = call(functools.partial(sum_body, cuts=cuts), [((SUB, E), BF16)] * 4, *got, flops=10**8)
    got = [pieces[0]] + [fetch(pieces[d], along_first(-d)) for d in (1, 2, 3)]
    cuts = [(0, 2 * OWN), (2 * OWN, 5 * OWN), (5 * OWN, 8 * OWN)]
    low, mid, high = call(
        functools.partial(sum_body, cuts=cuts), [((hi - lo, E), BF16) for lo, hi in cuts], *got, flops=10**8
    )
    low, high = fetch(low, along_z(2)), fetch(high, along_z(-3))
    before, own, after = call(
        near_body, [((OWN, E), BF16), ((OWN, E), F32), ((OWN, E), BF16)], mid, low, high, flops=10**8
    )
    before, after = fetch(before, along_z(1)), fetch(after, along_z(-1))
    return own + before.astype(F32) + after.astype(F32)


def on_device(image_features, head_weight, text_embeds, natural_exponent_factor, logit_bias):
    scalars = jnp.concatenate([jnp.exp(natural_exponent_factor), logit_bias])
    weight = gather_weight(head_weight)
    text_low, text_length = call(
        text_body, [((R, E), BF16), ((R, 1), F32)], text_embeds, flops=10**8
    )
    texts = [text_low]
    for _ in range(S - 1):
        texts.append(fetch(texts[-1], along_blocks(1)))
    pick, xp, xpt = call(
        order_body, [((D, D), BF16), ((R, D), BF16), ((D, R), BF16)], row_sources(), image_features,
        flops=4 * D * D * R,
    )
    full, unit, low, length = call(
        embed_body, [((D, E), BF16), ((R, E), F32), ((R, E), BF16), ((R, 1), F32)], xp, *weight,
        flops=2 * R * D * E,
    )
    images = [low]
    for _ in range(S - 1):
        images.append(fetch(images[-1], along_blocks(-1)))
    work = [pltpu.VMEM((R, E), F32), pltpu.VMEM((S, R, R), BF16)]
    eg, sent = call(
        image_body, [((R, E), BF16), ((HALF, E), BF16)], scalars, low, unit, length, *texts, xpt,
        flops=16 * R * R * E + 2 * R * HALF * E, scratch=work, smem=(0,),
    )
    came = fetch(sent, sibling)
    (grad_features,) = call(
        features_body, [((R, D), BF16)], eg, full, pick, flops=2 * R * D * E + 2 * R * D * D,
        scratch=[pltpu.VMEM((R, D), BF16)],
    )
    pieces = call(weight_body, [((PIECE, E), BF16)] * 4, xpt, eg, came, flops=2 * R * HALF * E)
    grad_weight = scatter_weight(pieces)
    (grad_text,) = call(
        text_grad_body, [((R, E), BF16)], scalars, text_embeds, text_low, text_length, *images,
        flops=16 * R * R * E, scratch=work, smem=(0,),
    )
    return grad_features, grad_text, grad_weight


def solution(mesh):
    finer = Mesh(mesh.devices.reshape(NY, NZ, NX, NC), AXES)
    rows = P(AXES, None)
    return jax.shard_map(
        on_device,
        mesh=finer,
        in_specs=(rows, rows, rows, P(), P()),
        out_specs=(rows, rows, rows),
        check_vma=False,
    )
```

```python
import functools

import jax
import jax.numpy as jnp
from jax import lax
from jax.experimental import pallas as pl
from jax.experimental.pallas import tpu as pltpu
from jax.sharding import Mesh
from jax.sharding import PartitionSpec as P


S = 4
EPS = 1e-06
NY, NZ, NX, NC = 4, 8, 4, 2
NDEV = NY * NZ * NX * NC
AXES = ("y", "z", "x", "c")
R, D, E = 256, 1536, 1152
HALF = D // 2
PIECE = HALF // 4
SUB = PIECE // 4
OWN = D // NDEV
F32, BF16 = jnp.float32, jnp.bfloat16
NN = (((1,), (0,)), ((), ()))
NT = (((1,), (1,)), ((), ()))
COLS = 384


def mm(a, b, dims=NN):
    return lax.dot_general(a, b, dims, preferred_element_type=F32)


def index(y, z, x, c):
    return ((y % NY * NZ + z % NZ) * NX + x % NX) * NC + c % NC


def coords(i):
    return i // (NZ * NX * NC), i // (NX * NC) % NZ, i // NC % NX, i % NC


def fetch(value, where):
    return lax.ppermute(value, AXES, [(index(*where(*coords(i))), i) for i in range(NDEV)])


def along_z(d):
    return lambda y, z, x, c: (y, z + d, x, c)


def along_first(d):
    return lambda y, z, x, c: (y, z, x + d, c) if c == 0 else (y + d, z, x, c)


def along_second(d):
    return lambda y, z, x, c: (y + d, z, x, c) if c == 0 else (y, z, x + d, c)


def sibling(y, z, x, c):
    return y, z, x, 1 - c


def along_blocks(d):
    return lambda y, z, x, c: coords((index(y, z, x, c) + d) % NDEV)


def call(body, outs, *args, flops=0, scratch=(), smem=(), limit=16):
    def spec(i):
        return pl.BlockSpec(memory_space=pltpu.SMEM if i in smem else pltpu.VMEM)

    return pl.pallas_call(
        body,
        out_shape=[pltpu.VMEM(s, d) for s, d in outs],
        in_specs=[spec(i) for i in range(len(args))],
        out_specs=[pl.BlockSpec(memory_space=pltpu.VMEM) for _ in outs],
        scratch_shapes=list(scratch),
        compiler_params=pltpu.CompilerParams(vmem_limit_bytes=limit << 20),
        cost_estimate=pl.CostEstimate(flops=flops, bytes_accessed=0, transcendentals=0),
    )(*(a if i in smem else pltpu.with_memory_space_constraint(a, pltpu.VMEM) for i, a in enumerate(args)))


def text_body(raw_ref, low_ref, length_ref):
    raw = raw_ref[...].astype(F32)
    length = jnp.sqrt(jnp.sum(raw * raw, axis=1, keepdims=True) + EPS)
    length_ref[...] = length
    low_ref[...] = (raw / length).astype(BF16)


def order_body(coord_ref, x_ref, pick_ref, xp_ref, xpt_ref):
    y, z, x, c = (coord_ref[i] for i in range(4))
    row = lax.broadcasted_iota(jnp.int32, (SUB, 1), 0)
    within = (z + row // OWN + (NZ - 3)) % NZ * (NX * NC * OWN) + row % OWN
    lanes = lax.broadcasted_iota(jnp.int32, (SUB, D), 1)

    @pl.loop(0, D // COLS)
    def _(i):
        for j in range(COLS // SUB):
            group = i * (COLS // SUB) + j
            core = (c + group // 16) % NC
            second, first = group // 4 % 4, group % 4
            at_y = (y + jnp.where(core == 0, second, first)) % NY
            at_x = (x + jnp.where(core == 0, first, second)) % NX
            base = (at_y * (NZ * NX * NC) + at_x * NC + core) * OWN
            chosen = jnp.where(lanes == within + base, 1.0, 0.0).astype(BF16)
            pick_ref[pl.ds(pl.multiple_of(i * COLS + j * SUB, 16), SUB), :] = chosen
        rows = pl.ds(pl.multiple_of(i * COLS, COLS), COLS)
        xpt_ref[rows, :] = mm(pick_ref[rows, :], x_ref[...], NT).astype(BF16)
        xp_ref[:, rows] = mm(x_ref[...], pick_ref[rows, :], NT).astype(BF16)


def embed_body(xp_ref, *refs):
    pieces, (w_ref, unit_ref, low_ref, length_ref) = refs[:8], refs[8:]
    for i, piece in enumerate(pieces):
        w_ref[pl.ds(i * PIECE, PIECE), :] = piece[...]
    squares = jnp.zeros((R, 1), F32)
    for at in range(0, E, COLS):
        cols = pl.ds(at, COLS)
        part = mm(xp_ref[...], w_ref[:, cols])
        unit_ref[:, cols] = part
        squares = squares + jnp.sum(part * part, axis=1, keepdims=True)
    length = jnp.sqrt(squares + EPS)
    length_ref[...] = length
    unit = unit_ref[...] / length
    unit_ref[...] = unit
    low_ref[...] = unit.astype(BF16)


def derivative(rows, columns, scale, bias, diagonal):
    logits = scale * mm(rows, columns, NT) + bias
    if not diagonal:
        return (scale * jax.nn.sigmoid(logits)).astype(BF16)
    matched = lax.broadcasted_iota(jnp.int32, logits.shape, 0) == lax.broadcasted_iota(
        jnp.int32, logits.shape, 1
    )
    polarity = jnp.where(matched, 1.0, -1.0)
    return (-scale * polarity * jax.nn.sigmoid(-polarity * logits)).astype(BF16)


def image_body(scalar_ref, low_ref, unit_ref, length_ref, t0, t1, t2, t3, xpt_ref, eg_ref, gw_ref, grad, pair):
    scale, bias = scalar_ref[0], scalar_ref[1]
    texts = (t0, t1, t2, t3)
    for k, text in enumerate(texts):
        pair[k] = derivative(low_ref[...], text[...], scale, bias, k == 0)
    inner = jnp.zeros((R, 1), F32)
    for at in range(0, E, COLS):
        cols = pl.ds(at, COLS)
        part = mm(pair[0], t0[:, cols])
        for k in range(1, S):
            part = part + mm(pair[k], texts[k][:, cols])
        grad[:, cols] = part
        inner = inner + jnp.sum(part * unit_ref[:, cols], axis=1, keepdims=True)
    eg_ref[...] = ((grad[...] - unit_ref[...] * inner) / length_ref[...]).astype(BF16)

    @pl.loop(0, HALF // PIECE)
    def _(i):
        at = pl.multiple_of(i * PIECE, PIECE)
        part = mm(xpt_ref[pl.ds(HALF + at, PIECE), :], eg_ref[...])
        gw_ref[pl.ds(at, PIECE), :] = part.astype(BF16)


def weight_body(xpt_ref, eg_ref, came_ref, *outs):
    for i, out in enumerate(outs):
        rows = pl.ds(i * PIECE, PIECE)
        out[...] = (mm(xpt_ref[rows, :], eg_ref[...]) + came_ref[rows, :].astype(F32)).astype(BF16)


def features_body(eg_ref, w_ref, pick_ref, out_ref, mixed):
    @pl.loop(0, D // COLS)
    def _(i):
        rows = pl.ds(pl.multiple_of(i * COLS, COLS), COLS)
        mixed[:, rows] = mm(eg_ref[...], w_ref[rows, :], NT).astype(BF16)

    @pl.loop(0, D // COLS)
    def _(i):
        cols = pl.ds(pl.multiple_of(i * COLS, COLS), COLS)
        out_ref[:, cols] = mm(mixed[...], pick_ref[:, cols]).astype(BF16)


def text_grad_body(scalar_ref, raw_ref, low_ref, length_ref, p0, p1, p2, p3, out_ref, grad, pair):
    scale, bias = scalar_ref[0], scalar_ref[1]
    images = (p0, p1, p2, p3)
    for k, image in enumerate(images):
        pair[k] = derivative(low_ref[...], image[...], scale, bias, k == 0)
    length = length_ref[...]
    inner = jnp.zeros((R, 1), F32)
    for at in range(0, E, COLS):
        cols = pl.ds(at, COLS)
        part = mm(pair[0], p0[:, cols])
        for k in range(1, S):
            part = part + mm(pair[k], images[k][:, cols])
        grad[:, cols] = part
        inner = inner + jnp.sum(part * (raw_ref[:, cols].astype(F32) / length), axis=1, keepdims=True)
    out_ref[...] = ((grad[...] - raw_ref[...].astype(F32) / length * inner) / length).astype(BF16)


def sum_body(*refs, cuts):
    ins, outs = refs[:4], refs[4:]
    total = ins[0][...].astype(F32)
    for ref in ins[1:]:
        total = total + ref[...].astype(F32)
    for out, (lo, hi) in zip(outs, cuts, strict=True):
        out[...] = total[lo:hi].astype(BF16)


def near_body(mid_ref, low_ref, high_ref, *outs):
    mid, low, high = (ref[...].astype(F32) for ref in (mid_ref, low_ref, high_ref))
    outs[0][...] = (mid[:OWN] + low[:OWN] + high[:OWN]).astype(BF16)
    outs[1][...] = mid[OWN : 2 * OWN] + low[OWN:] + high[OWN : 2 * OWN]
    outs[2][...] = (mid[2 * OWN :] + high[2 * OWN :]).astype(BF16)


def gather_weight(w):
    before, after = fetch(w, along_z(-1)), fetch(w, along_z(1))
    near = jnp.concatenate([before, w, after], 0)
    high, low = fetch(near, along_z(3)), fetch(near, along_z(-2))
    ring = jnp.concatenate([low[: 2 * OWN], near, high], 0)
    plane = [fetch(ring, along_first(d)) for d in (1, 2, 3)]
    plane = jnp.concatenate([ring] + plane, 0)
    half = [plane] + [fetch(plane, along_second(d)) for d in (1, 2, 3)]
    return half + [fetch(piece, sibling) for piece in half]


def scatter_weight(pieces):
    got = [pieces[0]] + [fetch(pieces[d], along_second(-d)) for d in (1, 2, 3)]
    cuts = [(i * SUB, (i + 1) * SUB) for i in range(4)]
    pieces = call(functools.partial(sum_body, cuts=cuts), [((SUB, E), BF16)] * 4, *got, flops=10**8)
    got = [pieces[0]] + [fetch(pieces[d], along_first(-d)) for d in (1, 2, 3)]
    cuts = [(0, 2 * OWN), (2 * OWN, 5 * OWN), (5 * OWN, 8 * OWN)]
    low, mid, high = call(
        functools.partial(sum_body, cuts=cuts), [((hi - lo, E), BF16) for lo, hi in cuts], *got, flops=10**8
    )
    high, low = fetch(high, along_z(-3)), fetch(low, along_z(2))
    before, own, after = call(
        near_body, [((OWN, E), BF16), ((OWN, E), F32), ((OWN, E), BF16)], mid, low, high, flops=10**8
    )
    before, after = fetch(before, along_z(1)), fetch(after, along_z(-1))
    return own + before.astype(F32) + after.astype(F32)


def on_device(image_features, head_weight, text_embeds, natural_exponent_factor, logit_bias):
    scalars = jnp.concatenate([jnp.exp(natural_exponent_factor), logit_bias])
    place = jnp.stack([lax.axis_index(a) for a in AXES]).astype(jnp.int32)
    weight = gather_weight(head_weight)
    text_low, text_length = call(
        text_body, [((R, E), BF16), ((R, 1), F32)], text_embeds, flops=10**8
    )
    texts = [text_low]
    for _ in range(1, S):
        texts.append(fetch(texts[-1], along_blocks(1)))
    pick, xp, xpt = call(
        order_body, [((D, D), BF16), ((R, D), BF16), ((D, R), BF16)], place, image_features,
        flops=4 * D * D * R, smem=(0,),
    )
    full, unit, low, length = call(
        embed_body, [((D, E), BF16), ((R, E), F32), ((R, E), BF16), ((R, 1), F32)], xp, *weight,
        flops=2 * R * D * E,
    )
    images = [low]
    for _ in range(1, S):
        images.append(fetch(images[-1], along_blocks(-1)))
    work = [pltpu.VMEM((R, E), F32), pltpu.VMEM((S, R, R), BF16)]
    eg, sent = call(
        image_body, [((R, E), BF16), ((HALF, E), BF16)], scalars, low, unit, length, *texts, xpt,
        flops=16 * R * R * E + 2 * R * HALF * E, scratch=work, smem=(0,),
    )
    came = fetch(sent, sibling)
    (grad_features,) = call(
        features_body, [((R, D), BF16)], eg, full, pick, flops=2 * R * D * E + 2 * R * D * D,
        scratch=[pltpu.VMEM((R, D), BF16)],
    )
    pieces = call(weight_body, [((PIECE, E), BF16)] * 4, xpt, eg, came, flops=2 * R * HALF * E)
    grad_weight = scatter_weight(pieces)
    (grad_text,) = call(
        text_grad_body, [((R, E), BF16)], scalars, text_embeds, text_low, text_length, *images,
        flops=16 * R * R * E, scratch=work, smem=(0,),
    )
    return grad_features, grad_text, grad_weight


def solution(mesh):
    finer = Mesh(mesh.devices.reshape(NY, NZ, NX, NC), AXES)
    rows = P(AXES, None)

    return jax.shard_map(
        on_device,
        mesh=finer,
        in_specs=(rows, rows, rows, P(), P()),
        out_specs=(rows, rows, rows),
        check_vma=False,
    )
```

```python
import functools

import jax
import jax.numpy as jnp
from jax import lax
from jax.experimental import pallas as pl
from jax.experimental.pallas import tpu as pltpu
from jax.sharding import Mesh
from jax.sharding import PartitionSpec as P


S = 4
EPS = 1e-06
NY, NZ, NX, NC = 4, 8, 4, 2
NDEV = NY * NZ * NX * NC
AXES = ("y", "z", "x", "c")
R, D, E = 256, 1536, 1152
HALF = D // 2
PIECE = HALF // 4
SUB = PIECE // 4
OWN = D // NDEV
F32, BF16 = jnp.float32, jnp.bfloat16
NN = (((1,), (0,)), ((), ()))
NT = (((1,), (1,)), ((), ()))
COLS = 384


def mm(a, b, dims=NN):
    return lax.dot_general(a, b, dims, preferred_element_type=F32)


def index(y, z, x, c):
    return ((y % NY * NZ + z % NZ) * NX + x % NX) * NC + c % NC


def coords(i):
    return i // (NZ * NX * NC), i // (NX * NC) % NZ, i // NC % NX, i % NC


def fetch(value, where):
    return lax.ppermute(value, AXES, [(index(*where(*coords(i))), i) for i in range(NDEV)])


def along_z(d):
    return lambda y, z, x, c: (y, z + d, x, c)


def along_first(d):
    return lambda y, z, x, c: (y, z, x + d, c) if c == 0 else (y + d, z, x, c)


def along_second(d):
    return lambda y, z, x, c: (y + d, z, x, c) if c == 0 else (y, z, x + d, c)


def sibling(y, z, x, c):
    return y, z, x, 1 - c


def along_blocks(d):
    return lambda y, z, x, c: coords((index(y, z, x, c) + d) % NDEV)


def call(body, outs, *args, flops=0, scratch=(), smem=(), hbm=(), limit=16, final=False):
    def spec(i):
        return pl.BlockSpec(memory_space=pltpu.SMEM if i in smem else pltpu.HBM if i in hbm else pltpu.VMEM)

    return pl.pallas_call(
        body,
        out_shape=[jax.ShapeDtypeStruct(s, d) if final else pltpu.VMEM(s, d) for s, d in outs],
        in_specs=[spec(i) for i in range(len(args))],
        out_specs=[pl.BlockSpec(memory_space=pltpu.VMEM) for _ in outs],
        scratch_shapes=list(scratch),
        compiler_params=pltpu.CompilerParams(vmem_limit_bytes=limit << 20),
        cost_estimate=pl.CostEstimate(flops=flops, bytes_accessed=0, transcendentals=0),
    )(*(
        a if i in smem else pltpu.with_memory_space_constraint(a, pltpu.HBM if i in hbm else pltpu.VMEM)
        for i, a in enumerate(args)
    ))


def text_body(raw_ref, w_ref, low_ref, length_ref, kept_ref):
    kept_ref[...] = w_ref[...]
    raw = raw_ref[...].astype(F32)
    length = jnp.sqrt(jnp.sum(raw * raw, axis=1, keepdims=True) + EPS)
    length_ref[...] = length
    low_ref[...] = (raw / length).astype(BF16)


def order_body(coord_ref, source_ref, pick_ref, xp_ref, xpt_ref, x_ref, done):
    copy = pltpu.make_async_copy(source_ref, x_ref, done)
    copy.start()
    y, z, x, c = (coord_ref[i] for i in range(4))
    row = lax.broadcasted_iota(jnp.int32, (SUB, 1), 0)
    within = (z + row // OWN + (NZ - 3)) % NZ * (NX * NC * OWN) + row % OWN
    lanes = lax.broadcasted_iota(jnp.int32, (SUB, D), 1)

    @pl.loop(0, D // COLS)
    def _(i):
        for j in range(COLS // SUB):
            group = i * (COLS // SUB) + j
            core = (c + group // 16) % NC
            second, first = group // 4 % 4, group % 4
            at_y = (y + jnp.where(core == 0, second, first)) % NY
            at_x = (x + jnp.where(core == 0, first, second)) % NX
            base = (at_y * (NZ * NX * NC) + at_x * NC + core) * OWN
            chosen = jnp.where(lanes == within + base, 1.0, 0.0).astype(BF16)
            pick_ref[pl.ds(pl.multiple_of(i * COLS + j * SUB, 16), SUB), :] = chosen

    copy.wait()

    @pl.loop(0, D // COLS)
    def _(i):
        rows = pl.ds(pl.multiple_of(i * COLS, COLS), COLS)
        xpt_ref[rows, :] = mm(pick_ref[rows, :], x_ref[...], NT).astype(BF16)
        xp_ref[:, rows] = mm(x_ref[...], pick_ref[rows, :], NT).astype(BF16)


def embed_body(xp_ref, *refs):
    pieces, (w_ref, unit_ref, low_ref, length_ref) = refs[:8], refs[8:]
    for i, piece in enumerate(pieces):
        w_ref[pl.ds(i * PIECE, PIECE), :] = piece[...]
    squares = jnp.zeros((R, 1), F32)
    for at in range(0, E, COLS):
        cols = pl.ds(at, COLS)
        part = mm(xp_ref[...], w_ref[:, cols])
        unit_ref[:, cols] = part
        squares = squares + jnp.sum(part * part, axis=1, keepdims=True)
    length = jnp.sqrt(squares + EPS)
    length_ref[...] = length
    unit = unit_ref[...] / length
    unit_ref[...] = unit
    low_ref[...] = unit.astype(BF16)


def derivative(rows, columns, scale, bias, diagonal):
    logits = scale * mm(rows, columns, NT) + bias
    if not diagonal:
        return (scale * jax.nn.sigmoid(logits)).astype(BF16)
    matched = lax.broadcasted_iota(jnp.int32, logits.shape, 0) == lax.broadcasted_iota(
        jnp.int32, logits.shape, 1
    )
    polarity = jnp.where(matched, 1.0, -1.0)
    return (-scale * polarity * jax.nn.sigmoid(-polarity * logits)).astype(BF16)


def image_body(scalar_ref, low_ref, unit_ref, length_ref, t0, t1, t2, t3, xpt_ref, eg_ref, s0, s1, s2, s3, grad, pair):
    scale, bias = scalar_ref[0], scalar_ref[1]
    texts = (t0, t1, t2, t3)
    for k, text in enumerate(texts):
        pair[k] = derivative(low_ref[...], text[...], scale, bias, k == 0)
    inner = jnp.zeros((R, 1), F32)
    for at in range(0, E, COLS):
        cols = pl.ds(at, COLS)
        part = mm(pair[0], t0[:, cols])
        for k in range(1, S):
            part = part + mm(pair[k], texts[k][:, cols])
        grad[:, cols] = part
        inner = inner + jnp.sum(part * unit_ref[:, cols], axis=1, keepdims=True)
    eg_ref[...] = ((grad[...] - unit_ref[...] * inner) / length_ref[...]).astype(BF16)
    for i, out in enumerate((s0, s1, s2, s3)):
        out[...] = mm(xpt_ref[pl.ds(HALF + i * PIECE, PIECE), :], eg_ref[...]).astype(BF16)


def weight_body(xpt_ref, eg_ref, came_ref, out, *, piece):
    rows = pl.ds(piece * PIECE, PIECE)
    out[...] = (mm(xpt_ref[rows, :], eg_ref[...]) + came_ref[...].astype(F32)).astype(BF16)


def join_body(*refs, rows):
    parts = [ref[...].astype(F32)[:n] for ref, n in zip(refs[:-1], rows, strict=True)]
    refs[-1][...] = jnp.concatenate(parts, 0).astype(BF16)


def stack_body(*refs):
    for i, ref in enumerate(refs[:-1]):
        refs[-1][pl.ds(i * SUB, SUB), :] = ref[...]


def features_body(eg_ref, w_ref, pick_ref, out_ref, mixed):
    @pl.loop(0, D // COLS)
    def _(i):
        rows = pl.ds(pl.multiple_of(i * COLS, COLS), COLS)
        mixed[:, rows] = mm(eg_ref[...], w_ref[rows, :], NT).astype(BF16)

    @pl.loop(0, D // COLS)
    def _(i):
        cols = pl.ds(pl.multiple_of(i * COLS, COLS), COLS)
        out_ref[:, cols] = mm(mixed[...], pick_ref[:, cols]).astype(BF16)


def text_grad_body(scalar_ref, raw_ref, low_ref, length_ref, p0, p1, p2, p3, out_ref, grad, pair):
    scale, bias = scalar_ref[0], scalar_ref[1]
    images = (p0, p1, p2, p3)
    for k, image in enumerate(images):
        pair[k] = derivative(low_ref[...], image[...], scale, bias, k == 0)
    length = length_ref[...]
    inner = jnp.zeros((R, 1), F32)
    for at in range(0, E, COLS):
        cols = pl.ds(at, COLS)
        part = mm(pair[0], p0[:, cols])
        for k in range(1, S):
            part = part + mm(pair[k], images[k][:, cols])
        grad[:, cols] = part
        inner = inner + jnp.sum(part * (raw_ref[:, cols].astype(F32) / length), axis=1, keepdims=True)
    out_ref[...] = ((grad[...] - raw_ref[...].astype(F32) / length * inner) / length).astype(BF16)


def sum_body(*refs, cuts):
    ins, outs = refs[:4], refs[4:]
    total = ins[0][...].astype(F32)
    for ref in ins[1:]:
        total = total + ref[...].astype(F32)
    for out, (lo, hi) in zip(outs, cuts, strict=True):
        out[...] = total[lo:hi].astype(BF16)


def near_body(mid_ref, low_ref, high_ref, *outs):
    mid, low, high = (ref[...].astype(F32) for ref in (mid_ref, low_ref, high_ref))
    outs[0][...] = (mid[:OWN] + low[:OWN] + high[:OWN]).astype(BF16)
    outs[1][...] = mid[OWN : 2 * OWN] + low[OWN:] + high[OWN : 2 * OWN]
    outs[2][...] = (mid[2 * OWN :] + high[2 * OWN :]).astype(BF16)


def join(rows, *parts):
    (out,) = call(functools.partial(join_body, rows=rows), [((sum(rows), E), BF16)], *parts, flops=10**6)
    return out


def gather_weight(kept, before, after):
    near = join((OWN,) * 3, before, kept, after)
    high, low = fetch(near, along_z(3)), fetch(near, along_z(-2))
    ring = join((2 * OWN, 3 * OWN, 3 * OWN), low, near, high)
    plane = [fetch(ring, along_first(d)) for d in (1, 2, 3)]
    (plane,) = call(stack_body, [((PIECE, E), BF16)], ring, *plane, flops=10**6)
    half = [plane] + [fetch(plane, along_second(d)) for d in (1, 2, 3)]
    return half + [fetch(piece, sibling) for piece in half]


def scatter_weight(pieces):
    got = [pieces[0]] + [fetch(pieces[d], along_second(-d)) for d in (1, 2, 3)]
    cuts = [(i * SUB, (i + 1) * SUB) for i in range(4)]
    pieces = call(functools.partial(sum_body, cuts=cuts), [((SUB, E), BF16)] * 4, *got, flops=10**8)
    got = [pieces[0]] + [fetch(pieces[d], along_first(-d)) for d in (1, 2, 3)]
    cuts = [(0, 2 * OWN), (2 * OWN, 5 * OWN), (5 * OWN, 8 * OWN)]
    low, mid, high = call(
        functools.partial(sum_body, cuts=cuts), [((hi - lo, E), BF16) for lo, hi in cuts], *got, flops=10**8
    )
    high, low = fetch(high, along_z(-3)), fetch(low, along_z(2))
    before, own, after = call(
        near_body, [((OWN, E), BF16), ((OWN, E), F32), ((OWN, E), BF16)], mid, low, high, flops=10**8
    )
    before, after = fetch(before, along_z(1)), fetch(after, along_z(-1))
    return own + before.astype(F32) + after.astype(F32)


def on_device(image_features, head_weight, text_embeds, natural_exponent_factor, logit_bias):
    scalars = jnp.concatenate([jnp.exp(natural_exponent_factor), logit_bias])
    place = jnp.stack([lax.axis_index(a) for a in AXES]).astype(jnp.int32)
    before = fetch(head_weight, along_z(-1))
    behind = fetch(head_weight, along_z(1))
    text_low, text_length, kept = call(
        text_body, [((R, E), BF16), ((R, 1), F32), ((OWN, E), BF16)], text_embeds, head_weight, flops=10**8
    )
    weight = gather_weight(kept, before, behind)
    text1 = fetch(text_low, along_blocks(1))
    text2 = fetch(text_low, along_blocks(2))
    text3 = fetch(text2, along_blocks(1))
    texts = [text_low, text1, text2, text3]
    pick, xp, xpt = call(
        order_body, [((D, D), BF16), ((R, D), BF16), ((D, R), BF16)], place, image_features,
        flops=4 * D * D * R, smem=(0,), hbm=(1,),
        scratch=[pltpu.VMEM((R, D), BF16), pltpu.SemaphoreType.DMA(())],
    )
    full, unit, low, length = call(
        embed_body, [((D, E), BF16), ((R, E), F32), ((R, E), BF16), ((R, 1), F32)], xp, *weight,
        flops=2 * R * D * E,
    )
    images = [low]
    for _ in range(1, S):
        images.append(fetch(images[-1], along_blocks(-1)))
    work = [pltpu.VMEM((R, E), F32), pltpu.VMEM((S, R, R), BF16)]
    eg, *sent = call(
        image_body, [((R, E), BF16)] + [((PIECE, E), BF16)] * 4, scalars, low, unit, length, *texts, xpt,
        flops=16 * R * R * E + 2 * R * HALF * E, scratch=work, smem=(0,),
    )
    came = [fetch(piece, sibling) for piece in sent]
    (grad_features,) = call(
        features_body, [((R, D), BF16)], eg, full, pick, flops=2 * R * D * E + 2 * R * D * D,
        scratch=[pltpu.VMEM((R, D), BF16)], final=True,
    )
    pieces = []
    for i in range(4):
        pieces += call(
            functools.partial(weight_body, piece=i), [((PIECE, E), BF16)], xpt, eg, came[i], flops=2 * R * PIECE * E
        )
    grad_weight = scatter_weight(pieces)
    (grad_text,) = call(
        text_grad_body, [((R, E), BF16)], scalars, text_embeds, text_low, text_length, *images,
        flops=16 * R * R * E, scratch=work, smem=(0,), final=True,
    )
    return grad_features, grad_text, grad_weight


def solution(mesh):
    finer = Mesh(mesh.devices.reshape(NY, NZ, NX, NC), AXES)
    rows = P(AXES, None)

    return jax.shard_map(
        on_device,
        mesh=finer,
        in_specs=(rows, rows, rows, P(), P()),
        out_specs=(rows, rows, rows),
        check_vma=False,
    )
```

```python
import functools

import jax
import jax.numpy as jnp
from jax import lax
from jax.experimental import pallas as pl
from jax.experimental.pallas import tpu as pltpu
from jax.sharding import Mesh
from jax.sharding import PartitionSpec as P


S = 4
EPS = 1e-06
NY, NZ, NX, NC = 4, 8, 4, 2
NDEV = NY * NZ * NX * NC
AXES = ("y", "z", "x", "c")
R, D, E = 256, 1536, 1152
HALF = D // 2
PIECE = HALF // 4
SUB = PIECE // 4
OWN = D // NDEV
F32, BF16 = jnp.float32, jnp.bfloat16
NN = (((1,), (0,)), ((), ()))
NT = (((1,), (1,)), ((), ()))
COLS = 384


def mm(a, b, dims=NN):
    return lax.dot_general(a, b, dims, preferred_element_type=F32)


def index(y, z, x, c):
    return ((y % NY * NZ + z % NZ) * NX + x % NX) * NC + c % NC


def coords(i):
    return i // (NZ * NX * NC), i // (NX * NC) % NZ, i // NC % NX, i % NC


def fetch(value, where):
    return lax.ppermute(value, AXES, [(index(*where(*coords(i))), i) for i in range(NDEV)])


def along_z(d):
    return lambda y, z, x, c: (y, z + d, x, c)


def along_first(d):
    return lambda y, z, x, c: (y, z, x + d, c) if c == 0 else (y + d, z, x, c)


def along_second(d):
    return lambda y, z, x, c: (y + d, z, x, c) if c == 0 else (y, z, x + d, c)


def sibling(y, z, x, c):
    return y, z, x, 1 - c


def send(value, step, parity):
    return lax.ppermute(value, AXES, [(i, (i + step) % NDEV) for i in range(parity, NDEV, 2)])


def window(own, step):
    inner, outer = (1, 0) if step < 0 else (0, 1)

    def near(value):
        return send(value, step, inner)

    def far(value):
        return send(value, step, outer)

    a1, b1 = near(own), far(own)
    b2, a2 = far(a1), near(b1)
    b3, a3 = far(a2), near(b2)
    return a1, a2, a3, b1, b2, b3


def call(body, outs, *args, flops=0, scratch=(), smem=(), hbm=(), limit=16, final=False):
    def spec(i):
        return pl.BlockSpec(memory_space=pltpu.SMEM if i in smem else pltpu.HBM if i in hbm else pltpu.VMEM)

    return pl.pallas_call(
        body,
        out_shape=[jax.ShapeDtypeStruct(s, d) if final else pltpu.VMEM(s, d) for s, d in outs],
        in_specs=[spec(i) for i in range(len(args))],
        out_specs=[pl.BlockSpec(memory_space=pltpu.VMEM) for _ in outs],
        scratch_shapes=list(scratch),
        compiler_params=pltpu.CompilerParams(vmem_limit_bytes=limit << 20),
        cost_estimate=pl.CostEstimate(flops=flops, bytes_accessed=0, transcendentals=0),
    )(*(
        a if i in smem else pltpu.with_memory_space_constraint(a, pltpu.HBM if i in hbm else pltpu.VMEM)
        for i, a in enumerate(args)
    ))


def text_body(raw_ref, w_ref, low_ref, length_ref, kept_ref):
    kept_ref[...] = w_ref[...]
    raw = raw_ref[...].astype(F32)
    length = jnp.sqrt(jnp.sum(raw * raw, axis=1, keepdims=True) + EPS)
    length_ref[...] = length
    low_ref[...] = (raw / length).astype(BF16)


def order_body(coord_ref, source_ref, pick_ref, xp_ref, xpt_ref, x_ref, done):
    copy = pltpu.make_async_copy(source_ref, x_ref, done)
    copy.start()
    y, z, x, c = (coord_ref[i] for i in range(4))
    row = lax.broadcasted_iota(jnp.int32, (SUB, 1), 0)
    within = (z + row // OWN + (NZ - 3)) % NZ * (NX * NC * OWN) + row % OWN
    lanes = lax.broadcasted_iota(jnp.int32, (SUB, D), 1)

    @pl.loop(0, D // COLS)
    def _(i):
        for j in range(COLS // SUB):
            group = i * (COLS // SUB) + j
            core = (c + group // 16) % NC
            second, first = group // 4 % 4, group % 4
            at_y = (y + jnp.where(core == 0, second, first)) % NY
            at_x = (x + jnp.where(core == 0, first, second)) % NX
            base = (at_y * (NZ * NX * NC) + at_x * NC + core) * OWN
            chosen = jnp.where(lanes == within + base, 1.0, 0.0).astype(BF16)
            pick_ref[pl.ds(pl.multiple_of(i * COLS + j * SUB, 16), SUB), :] = chosen

    copy.wait()

    @pl.loop(0, D // COLS)
    def _(i):
        rows = pl.ds(pl.multiple_of(i * COLS, COLS), COLS)
        xpt_ref[rows, :] = mm(pick_ref[rows, :], x_ref[...], NT).astype(BF16)
        xp_ref[:, rows] = mm(x_ref[...], pick_ref[rows, :], NT).astype(BF16)


def embed_body(xp_ref, *refs):
    pieces, (w_ref, unit_ref, low_ref, length_ref) = refs[:8], refs[8:]
    for i, piece in enumerate(pieces):
        w_ref[pl.ds(i * PIECE, PIECE), :] = piece[...]
    squares = jnp.zeros((R, 1), F32)
    for at in range(0, E, COLS):
        cols = pl.ds(at, COLS)
        part = mm(xp_ref[...], w_ref[:, cols])
        unit_ref[:, cols] = part
        squares = squares + jnp.sum(part * part, axis=1, keepdims=True)
    length = jnp.sqrt(squares + EPS)
    length_ref[...] = length
    unit = unit_ref[...] / length
    unit_ref[...] = unit
    low_ref[...] = unit.astype(BF16)


def derivative(rows, columns, scale, bias, diagonal):
    logits = scale * mm(rows, columns, NT) + bias
    if not diagonal:
        return (scale * jax.nn.sigmoid(logits)).astype(BF16)
    matched = lax.broadcasted_iota(jnp.int32, logits.shape, 0) == lax.broadcasted_iota(
        jnp.int32, logits.shape, 1
    )
    polarity = jnp.where(matched, 1.0, -1.0)
    return (-scale * polarity * jax.nn.sigmoid(-polarity * logits)).astype(BF16)


def collect(all_ref, refs, near):
    all_ref[pl.ds(0, R), :] = refs[0][...]

    @pl.when(near)
    def _():
        for k in range(1, S):
            all_ref[pl.ds(k * R, R), :] = refs[k][...]

    @pl.when(jnp.logical_not(near))
    def _():
        for k in range(1, S):
            all_ref[pl.ds(k * R, R), :] = refs[k + S - 1][...]


def image_body(
    scalar_ref, coord_ref, low_ref, unit_ref, length_ref, *refs
):
    text_refs, (xpt_ref, eg_ref, s0, s1, s2, s3, grad, pair, texts) = refs[:7], refs[7:]
    scale, bias = scalar_ref[0], scalar_ref[1]
    collect(texts, text_refs, coord_ref[3] == 0)
    for k in range(S):
        rows = pl.ds(k * R, R)
        pair[:, rows] = derivative(low_ref[...], texts[rows, :], scale, bias, k == 0)
    inner = jnp.zeros((R, 1), F32)
    for at in range(0, E, COLS):
        cols = pl.ds(at, COLS)
        part = mm(pair[...], texts[:, cols])
        grad[:, cols] = part
        inner = inner + jnp.sum(part * unit_ref[:, cols], axis=1, keepdims=True)
    eg_ref[...] = ((grad[...] - unit_ref[...] * inner) / length_ref[...]).astype(BF16)
    for i, out in enumerate((s0, s1, s2, s3)):
        out[...] = mm(xpt_ref[pl.ds(HALF + i * PIECE, PIECE), :], eg_ref[...]).astype(BF16)


def weight_body(xpt_ref, eg_ref, came_ref, out, *, piece):
    rows = pl.ds(piece * PIECE, PIECE)
    out[...] = (mm(xpt_ref[rows, :], eg_ref[...]) + came_ref[...].astype(F32)).astype(BF16)


def join_body(*refs, rows):
    parts = [ref[...].astype(F32)[:n] for ref, n in zip(refs[:-1], rows, strict=True)]
    refs[-1][...] = jnp.concatenate(parts, 0).astype(BF16)


def stack_body(*refs):
    for i, ref in enumerate(refs[:-1]):
        refs[-1][pl.ds(i * SUB, SUB), :] = ref[...]


def features_body(eg_ref, w_ref, pick_ref, out_ref, mixed):
    @pl.loop(0, D // COLS)
    def _(i):
        rows = pl.ds(pl.multiple_of(i * COLS, COLS), COLS)
        mixed[:, rows] = mm(eg_ref[...], w_ref[rows, :], NT).astype(BF16)

    @pl.loop(0, D // COLS)
    def _(i):
        cols = pl.ds(pl.multiple_of(i * COLS, COLS), COLS)
        out_ref[:, cols] = mm(mixed[...], pick_ref[:, cols]).astype(BF16)


def text_grad_body(scalar_ref, coord_ref, raw_ref, low_ref, length_ref, *refs):
    image_refs, (out_ref, grad, pair, images) = refs[:7], refs[7:]
    scale, bias = scalar_ref[0], scalar_ref[1]
    collect(images, image_refs, coord_ref[3] == 1)
    for k in range(S):
        rows = pl.ds(k * R, R)
        pair[:, rows] = derivative(low_ref[...], images[rows, :], scale, bias, k == 0)
    length = length_ref[...]
    inner = jnp.zeros((R, 1), F32)
    for at in range(0, E, COLS):
        cols = pl.ds(at, COLS)
        part = mm(pair[...], images[:, cols])
        grad[:, cols] = part
        inner = inner + jnp.sum(part * (raw_ref[:, cols].astype(F32) / length), axis=1, keepdims=True)
    out_ref[...] = ((grad[...] - raw_ref[...].astype(F32) / length * inner) / length).astype(BF16)


def sum_body(*refs, cuts):
    ins, outs = refs[:4], refs[4:]
    total = ins[0][...].astype(F32)
    for ref in ins[1:]:
        total = total + ref[...].astype(F32)
    for out, (lo, hi) in zip(outs, cuts, strict=True):
        out[...] = total[lo:hi].astype(BF16)


def near_body(mid_ref, low_ref, high_ref, *outs):
    mid, low, high = (ref[...].astype(F32) for ref in (mid_ref, low_ref, high_ref))
    outs[0][...] = (mid[:OWN] + low[:OWN] + high[:OWN]).astype(BF16)
    outs[1][...] = mid[OWN : 2 * OWN] + low[OWN:] + high[OWN : 2 * OWN]
    outs[2][...] = (mid[2 * OWN :] + high[2 * OWN :]).astype(BF16)


def join(rows, *parts):
    (out,) = call(functools.partial(join_body, rows=rows), [((sum(rows), E), BF16)], *parts, flops=10**6)
    return out


def gather_weight(kept, before, after):
    near = join((OWN,) * 3, before, kept, after)
    high, low = fetch(near, along_z(3)), fetch(near, along_z(-2))
    ring = join((2 * OWN, 3 * OWN, 3 * OWN), low, near, high)
    plane = [fetch(ring, along_first(d)) for d in (1, 2, 3)]
    (plane,) = call(stack_body, [((PIECE, E), BF16)], ring, *plane, flops=10**6)
    half = [plane] + [fetch(plane, along_second(d)) for d in (1, 2, 3)]
    return half + [fetch(piece, sibling) for piece in half]


def scatter_weight(pieces):
    got = [pieces[0]] + [fetch(pieces[d], along_second(-d)) for d in (1, 2, 3)]
    cuts = [(i * SUB, (i + 1) * SUB) for i in range(4)]
    pieces = call(functools.partial(sum_body, cuts=cuts), [((SUB, E), BF16)] * 4, *got, flops=10**8)
    got = [pieces[0]] + [fetch(pieces[d], along_first(-d)) for d in (1, 2, 3)]
    cuts = [(0, 2 * OWN), (2 * OWN, 5 * OWN), (5 * OWN, 8 * OWN)]
    low, mid, high = call(
        functools.partial(sum_body, cuts=cuts), [((hi - lo, E), BF16) for lo, hi in cuts], *got, flops=10**8
    )
    high, low = fetch(high, along_z(-3)), fetch(low, along_z(2))
    before, own, after = call(
        near_body, [((OWN, E), BF16), ((OWN, E), F32), ((OWN, E), BF16)], mid, low, high, flops=10**8
    )
    before, after = fetch(before, along_z(1)), fetch(after, along_z(-1))
    return own + before.astype(F32) + after.astype(F32)


def on_device(image_features, head_weight, text_embeds, natural_exponent_factor, logit_bias):
    scalars = jnp.concatenate([jnp.exp(natural_exponent_factor), logit_bias])
    place = jnp.stack([lax.axis_index(a) for a in AXES]).astype(jnp.int32)
    before = fetch(head_weight, along_z(-1))
    behind = fetch(head_weight, along_z(1))
    text_low, text_length, kept = call(
        text_body, [((R, E), BF16), ((R, 1), F32), ((OWN, E), BF16)], text_embeds, head_weight, flops=10**8
    )
    weight = gather_weight(kept, before, behind)
    texts = (text_low, *window(text_low, -1))
    pick, xp, xpt = call(
        order_body, [((D, D), BF16), ((R, D), BF16), ((D, R), BF16)], place, image_features,
        flops=4 * D * D * R, smem=(0,), hbm=(1,),
        scratch=[pltpu.VMEM((R, D), BF16), pltpu.SemaphoreType.DMA(())],
    )
    full, unit, low, length = call(
        embed_body, [((D, E), BF16), ((R, E), F32), ((R, E), BF16), ((R, 1), F32)], xp, *weight,
        flops=2 * R * D * E,
    )
    images = (low, *window(low, 1))
    work = [pltpu.VMEM((R, E), F32), pltpu.VMEM((R, S * R), BF16), pltpu.VMEM((S * R, E), BF16)]
    eg, *sent = call(
        image_body, [((R, E), BF16)] + [((PIECE, E), BF16)] * 4, scalars, place, low, unit, length, *texts, xpt,
        flops=16 * R * R * E + 2 * R * HALF * E, scratch=work, smem=(0, 1),
    )
    came = [fetch(piece, sibling) for piece in sent]
    (grad_features,) = call(
        features_body, [((R, D), BF16)], eg, full, pick, flops=2 * R * D * E + 2 * R * D * D,
        scratch=[pltpu.VMEM((R, D), BF16)], final=True,
    )
    pieces = []
    for i in range(4):
        pieces += call(
            functools.partial(weight_body, piece=i), [((PIECE, E), BF16)], xpt, eg, came[i], flops=2 * R * PIECE * E
        )
    grad_weight = scatter_weight(pieces)
    (grad_text,) = call(
        text_grad_body, [((R, E), BF16)], scalars, place, text_embeds, text_low, text_length, *images,
        flops=16 * R * R * E, scratch=work, smem=(0, 1), final=True,
    )
    return grad_features, grad_text, grad_weight


def solution(mesh):
    finer = Mesh(mesh.devices.reshape(NY, NZ, NX, NC), AXES)
    rows = P(AXES, None)

    return jax.shard_map(
        on_device,
        mesh=finer,
        in_specs=(rows, rows, rows, P(), P()),
        out_specs=(rows, rows, rows),
        check_vma=False,
    )
```

```python
import functools

import jax
import jax.numpy as jnp
from jax import lax
from jax.experimental import pallas as pl
from jax.experimental.pallas import tpu as pltpu
from jax.sharding import Mesh
from jax.sharding import PartitionSpec as P


S = 4
EPS = 1e-06
NY, NZ, NX, NC = 4, 8, 4, 2
NDEV = NY * NZ * NX * NC
AXES = ("y", "z", "x", "c")
R, D, E = 256, 1536, 1152
HALF = D // 2
PIECE = HALF // 4
SUB = PIECE // 4
OWN = D // NDEV
F32, BF16 = jnp.float32, jnp.bfloat16
NN = (((1,), (0,)), ((), ()))
NT = (((1,), (1,)), ((), ()))
COLS = 384


def mm(a, b, dims=NN):
    return lax.dot_general(a, b, dims, preferred_element_type=F32)


def index(y, z, x, c):
    return ((y % NY * NZ + z % NZ) * NX + x % NX) * NC + c % NC


def coords(i):
    return i // (NZ * NX * NC), i // (NX * NC) % NZ, i // NC % NX, i % NC


def fetch(value, where):
    return lax.ppermute(value, AXES, [(index(*where(*coords(i))), i) for i in range(NDEV)])


def along_z(d):
    return lambda y, z, x, c: (y, z + d, x, c)


def along_first(d):
    return lambda y, z, x, c: (y, z, x + d, c) if c == 1 else (y + d, z, x, c)


def along_second(d):
    return lambda y, z, x, c: (y + d, z, x, c) if c == 1 else (y, z, x + d, c)


def sibling(y, z, x, c):
    return y, z, x, 1 - c


def along_blocks(d):
    return lambda y, z, x, c: coords((index(y, z, x, c) + d) % NDEV)


def call(body, outs, *args, flops=0, scratch=(), smem=(), hbm=(), limit=16, final=False):
    def spec(i):
        return pl.BlockSpec(memory_space=pltpu.SMEM if i in smem else pltpu.HBM if i in hbm else pltpu.VMEM)

    return pl.pallas_call(
        body,
        out_shape=[jax.ShapeDtypeStruct(s, d) if final else pltpu.VMEM(s, d) for s, d in outs],
        in_specs=[spec(i) for i in range(len(args))],
        out_specs=[pl.BlockSpec(memory_space=pltpu.VMEM) for _ in outs],
        scratch_shapes=list(scratch),
        compiler_params=pltpu.CompilerParams(vmem_limit_bytes=limit << 20),
        cost_estimate=pl.CostEstimate(flops=flops, bytes_accessed=0, transcendentals=0),
    )(*(
        a if i in smem else pltpu.with_memory_space_constraint(a, pltpu.HBM if i in hbm else pltpu.VMEM)
        for i, a in enumerate(args)
    ))


def length_of(rows):
    return jnp.sqrt(jnp.sum(rows * rows, axis=1, keepdims=True) + EPS)


def text_body(raw_source, w_source, low_ref, raw_ref, w_ref, done):
    half = R // 2
    copies = [pltpu.make_async_copy(w_source, w_ref, done.at[2])]
    for i in range(2):
        rows = pl.ds(i * half, half)
        copies.append(pltpu.make_async_copy(raw_source.at[rows, :], raw_ref.at[rows, :], done.at[i]))
    for copy in copies:
        copy.start()
    for i in range(2):
        rows = pl.ds(i * half, half)
        copies[i + 1].wait()
        raw = raw_ref[rows, :].astype(F32)
        low_ref[rows, :] = (raw / length_of(raw)).astype(BF16)
    copies[0].wait()


def order_body(coord_ref, source_ref, pick_ref, xp_ref, xpt_ref, x_ref, done):
    copy = pltpu.make_async_copy(source_ref, x_ref, done)
    copy.start()
    y, z, x, c = (coord_ref[i] for i in range(4))
    row = lax.broadcasted_iota(jnp.int32, (SUB, 1), 0)
    within = (z + row // OWN + (NZ - 3)) % NZ * (NX * NC * OWN) + row % OWN
    lanes = lax.broadcasted_iota(jnp.int32, (SUB, D), 1)

    @pl.loop(0, D // COLS)
    def _(i):
        for j in range(COLS // SUB):
            group = i * (COLS // SUB) + j
            core = (c + group // 16) % NC
            second, first = group // 4 % 4, group % 4
            at_y = (y + jnp.where(core == 1, second, first)) % NY
            at_x = (x + jnp.where(core == 1, first, second)) % NX
            base = (at_y * (NZ * NX * NC) + at_x * NC + core) * OWN
            chosen = jnp.where(lanes == within + base, 1.0, 0.0).astype(BF16)
            pick_ref[pl.ds(pl.multiple_of(i * COLS + j * SUB, 16), SUB), :] = chosen

    copy.wait()

    @pl.loop(0, D // COLS)
    def _(i):
        rows = pl.ds(pl.multiple_of(i * COLS, COLS), COLS)
        xpt_ref[rows, :] = mm(pick_ref[rows, :], x_ref[...], NT).astype(BF16)
        xp_ref[:, rows] = mm(x_ref[...], pick_ref[rows, :], NT).astype(BF16)


def embed_body(xp_ref, *refs):
    pieces, (w_ref, unit_ref, low_ref, length_ref) = refs[:8], refs[8:]
    for i, piece in enumerate(pieces):
        w_ref[pl.ds(i * PIECE, PIECE), :] = piece[...]
    squares = jnp.zeros((R, 1), F32)
    for at in range(0, E, COLS):
        cols = pl.ds(at, COLS)
        part = mm(xp_ref[...], w_ref[:, cols])
        unit_ref[:, cols] = part
        squares = squares + jnp.sum(part * part, axis=1, keepdims=True)
    length = jnp.sqrt(squares + EPS)
    length_ref[...] = length
    unit = unit_ref[...] / length
    unit_ref[...] = unit
    low_ref[...] = unit.astype(BF16)


def derivative(rows, columns, scale, bias, diagonal):
    logits = scale * mm(rows, columns, NT) + bias
    if not diagonal:
        return (scale * jax.nn.sigmoid(logits)).astype(BF16)
    matched = lax.broadcasted_iota(jnp.int32, logits.shape, 0) == lax.broadcasted_iota(
        jnp.int32, logits.shape, 1
    )
    polarity = jnp.where(matched, 1.0, -1.0)
    return (-scale * polarity * jax.nn.sigmoid(-polarity * logits)).astype(BF16)


def image_body(scalar_ref, low_ref, unit_ref, length_ref, t0, t1, t2, t3, xpt_ref, eg_ref, s0, s1, s2, s3, grad, pair):
    scale, bias = scalar_ref[0], scalar_ref[1]
    texts = (t0, t1, t2, t3)
    for k, text in enumerate(texts):
        pair[k] = derivative(low_ref[...], text[...], scale, bias, k == 0)
    inner = jnp.zeros((R, 1), F32)
    for at in range(0, E, COLS):
        cols = pl.ds(at, COLS)
        part = mm(pair[0], t0[:, cols])
        for k in range(1, S):
            part = part + mm(pair[k], texts[k][:, cols])
        grad[:, cols] = part
        inner = inner + jnp.sum(part * unit_ref[:, cols], axis=1, keepdims=True)
    eg_ref[...] = ((grad[...] - unit_ref[...] * inner) / length_ref[...]).astype(BF16)
    for i, out in enumerate((s0, s1, s2, s3)):
        out[...] = mm(xpt_ref[pl.ds(HALF + i * PIECE, PIECE), :], eg_ref[...]).astype(BF16)


def weight_body(xpt_ref, eg_ref, came_ref, out, *, piece):
    rows = pl.ds(piece * PIECE, PIECE)
    out[...] = (mm(xpt_ref[rows, :], eg_ref[...]) + came_ref[...].astype(F32)).astype(BF16)


def join_body(*refs, rows):
    parts = [ref[...].astype(F32)[:n] for ref, n in zip(refs[:-1], rows, strict=True)]
    refs[-1][...] = jnp.concatenate(parts, 0).astype(BF16)


def stack_body(*refs):
    for i, ref in enumerate(refs[:-1]):
        refs[-1][pl.ds(i * SUB, SUB), :] = ref[...]


def features_body(eg_ref, w_ref, pick_ref, out_ref, mixed):
    @pl.loop(0, D // COLS)
    def _(i):
        rows = pl.ds(pl.multiple_of(i * COLS, COLS), COLS)
        mixed[:, rows] = mm(eg_ref[...], w_ref[rows, :], NT).astype(BF16)

    @pl.loop(0, D // COLS)
    def _(i):
        cols = pl.ds(pl.multiple_of(i * COLS, COLS), COLS)
        out_ref[:, cols] = mm(mixed[...], pick_ref[:, cols]).astype(BF16)


def text_grad_body(scalar_ref, raw_ref, low_ref, p0, p1, p2, p3, out_ref, grad, pair):
    scale, bias = scalar_ref[0], scalar_ref[1]
    images = (p0, p1, p2, p3)
    for k, image in enumerate(images):
        pair[k] = derivative(low_ref[...], image[...], scale, bias, k == 0)
    length = length_of(raw_ref[...].astype(F32))
    inner = jnp.zeros((R, 1), F32)
    for at in range(0, E, COLS):
        cols = pl.ds(at, COLS)
        part = mm(pair[0], p0[:, cols])
        for k in range(1, S):
            part = part + mm(pair[k], images[k][:, cols])
        grad[:, cols] = part
        inner = inner + jnp.sum(part * (raw_ref[:, cols].astype(F32) / length), axis=1, keepdims=True)
    out_ref[...] = ((grad[...] - raw_ref[...].astype(F32) / length * inner) / length).astype(BF16)


def sum_body(*refs, cuts):
    ins, outs = refs[:4], refs[4:]
    total = ins[0][...].astype(F32)
    for ref in ins[1:]:
        total = total + ref[...].astype(F32)
    for out, (lo, hi) in zip(outs, cuts, strict=True):
        out[...] = total[lo:hi].astype(BF16)


def near_body(mid_ref, low_ref, high_ref, *outs):
    mid, low, high = (ref[...].astype(F32) for ref in (mid_ref, low_ref, high_ref))
    outs[0][...] = (mid[:OWN] + low[:OWN] + high[:OWN]).astype(BF16)
    outs[1][...] = mid[OWN : 2 * OWN] + low[OWN:] + high[OWN : 2 * OWN]
    outs[2][...] = (mid[2 * OWN :] + high[2 * OWN :]).astype(BF16)


def join(rows, *parts):
    (out,) = call(functools.partial(join_body, rows=rows), [((sum(rows), E), BF16)], *parts, flops=10**6)
    return out


def gather_weight(kept, before, after):
    near = join((OWN,) * 3, before, kept, after)
    high, low = fetch(near, along_z(3)), fetch(near, along_z(-2))
    ring = join((2 * OWN, 3 * OWN, 3 * OWN), low, near, high)
    plane = [fetch(ring, along_first(d)) for d in (1, 2, 3)]
    (plane,) = call(stack_body, [((PIECE, E), BF16)], ring, *plane, flops=10**6)
    half = [plane] + [fetch(plane, along_second(d)) for d in (1, 2, 3)]
    return half + [fetch(piece, sibling) for piece in half]


def scatter_weight(pieces):
    got = [pieces[0]] + [fetch(pieces[d], along_second(-d)) for d in (1, 2, 3)]
    cuts = [(i * SUB, (i + 1) * SUB) for i in range(4)]
    pieces = call(functools.partial(sum_body, cuts=cuts), [((SUB, E), BF16)] * 4, *got, flops=10**8)
    got = [pieces[0]] + [fetch(pieces[d], along_first(-d)) for d in (1, 2, 3)]
    cuts = [(0, 2 * OWN), (2 * OWN, 5 * OWN), (5 * OWN, 8 * OWN)]
    low, mid, high = call(
        functools.partial(sum_body, cuts=cuts), [((hi - lo, E), BF16) for lo, hi in cuts], *got, flops=10**8
    )
    high, low = fetch(high, along_z(-3)), fetch(low, along_z(2))
    before, own, after = call(
        near_body, [((OWN, E), BF16), ((OWN, E), F32), ((OWN, E), BF16)], mid, low, high, flops=10**8
    )
    before, after = fetch(before, along_z(1)), fetch(after, along_z(-1))
    return own + before.astype(F32) + after.astype(F32)


def on_device(image_features, head_weight, text_embeds, natural_exponent_factor, logit_bias):
    scalars = jnp.concatenate([jnp.exp(natural_exponent_factor), logit_bias])
    place = jnp.stack([lax.axis_index(a) for a in AXES]).astype(jnp.int32)
    before = fetch(head_weight, along_z(-1))
    behind = fetch(head_weight, along_z(1))
    text_low, text_raw, kept = call(
        text_body, [((R, E), BF16), ((R, E), BF16), ((OWN, E), BF16)], text_embeds, head_weight,
        flops=10**8, hbm=(0, 1), scratch=[pltpu.SemaphoreType.DMA((3,))],
    )
    weight = gather_weight(kept, before, behind)
    texts = [text_low]
    for _ in range(1, S):
        texts.append(fetch(texts[-1], along_blocks(1)))
    pick, xp, xpt = call(
        order_body, [((D, D), BF16), ((R, D), BF16), ((D, R), BF16)], place, image_features,
        flops=4 * D * D * R, smem=(0,), hbm=(1,),
        scratch=[pltpu.VMEM((R, D), BF16), pltpu.SemaphoreType.DMA(())],
    )
    full, unit, low, length = call(
        embed_body, [((D, E), BF16), ((R, E), F32), ((R, E), BF16), ((R, 1), F32)], xp, *weight,
        flops=2 * R * D * E,
    )
    images = [low]
    for _ in range(1, S):
        images.append(fetch(images[-1], along_blocks(-1)))
    work = [pltpu.VMEM((R, E), F32), pltpu.VMEM((S, R, R), BF16)]
    eg, *sent = call(
        image_body, [((R, E), BF16)] + [((PIECE, E), BF16)] * 4, scalars, low, unit, length, *texts, xpt,
        flops=16 * R * R * E + 2 * R * HALF * E, scratch=work, smem=(0,),
    )
    came = [fetch(piece, sibling) for piece in sent]
    (grad_features,) = call(
        features_body, [((R, D), BF16)], eg, full, pick, flops=2 * R * D * E + 2 * R * D * D,
        scratch=[pltpu.VMEM((R, D), BF16)], final=True,
    )
    pieces = []
    for i in range(4):
        pieces += call(
            functools.partial(weight_body, piece=i), [((PIECE, E), BF16)], xpt, eg, came[i], flops=2 * R * PIECE * E
        )
    grad_weight = scatter_weight(pieces)
    (grad_text,) = call(
        text_grad_body, [((R, E), BF16)], scalars, text_raw, text_low, *images,
        flops=16 * R * R * E, scratch=work, smem=(0,), final=True,
    )
    return grad_features, grad_text, grad_weight


def solution(mesh):
    finer = Mesh(mesh.devices.reshape(NY, NZ, NX, NC), AXES)
    rows = P(AXES, None)

    return jax.shard_map(
        on_device,
        mesh=finer,
        in_specs=(rows, rows, rows, P(), P()),
        out_specs=(rows, rows, rows),
        check_vma=False,
    )
```

```python
import functools

import jax
import jax.numpy as jnp
from jax import lax
from jax.experimental import pallas as pl
from jax.experimental.pallas import tpu as pltpu
from jax.sharding import Mesh
from jax.sharding import PartitionSpec as P


S = 4
EPS = 1e-06
NY, NZ, NX, NC = 4, 8, 4, 2
NDEV = NY * NZ * NX * NC
AXES = ("y", "z", "x", "c")
R, D, E = 256, 1536, 1152
HALF = D // 2
PIECE = HALF // 4
SUB = PIECE // 4
OWN = D // NDEV
F32, BF16 = jnp.float32, jnp.bfloat16
NN = (((1,), (0,)), ((), ()))
NT = (((1,), (1,)), ((), ()))
COLS = 384


def mm(a, b, dims=NN):
    return lax.dot_general(a, b, dims, preferred_element_type=F32)


def index(y, z, x, c):
    return ((y % NY * NZ + z % NZ) * NX + x % NX) * NC + c % NC


def coords(i):
    return i // (NZ * NX * NC), i // (NX * NC) % NZ, i // NC % NX, i % NC


def fetch(value, where):
    return lax.ppermute(value, AXES, [(index(*where(*coords(i))), i) for i in range(NDEV)])


def along_z(d):
    return lambda y, z, x, c: (y, z + d, x, c)


def along_first(d):
    return lambda y, z, x, c: (y, z, x + d, c) if c == 0 else (y + d, z, x, c)


def along_second(d):
    return lambda y, z, x, c: (y + d, z, x, c) if c == 0 else (y, z, x + d, c)


def sibling(y, z, x, c):
    return y, z, x, 1 - c


def along_blocks(d):
    return lambda y, z, x, c: coords((index(y, z, x, c) + d) % NDEV)


def call(body, outs, *args, flops=0, scratch=(), smem=(), hbm=(), limit=8, final=False):
    def spec(i):
        return pl.BlockSpec(memory_space=pltpu.SMEM if i in smem else pltpu.HBM if i in hbm else pltpu.VMEM)

    return pl.pallas_call(
        body,
        out_shape=[jax.ShapeDtypeStruct(s, d) if final else pltpu.VMEM(s, d) for s, d in outs],
        in_specs=[spec(i) for i in range(len(args))],
        out_specs=[pl.BlockSpec(memory_space=pltpu.VMEM) for _ in outs],
        scratch_shapes=list(scratch),
        compiler_params=pltpu.CompilerParams(vmem_limit_bytes=limit << 20),
        cost_estimate=pl.CostEstimate(flops=flops, bytes_accessed=0, transcendentals=0),
    )(*(
        a if i in smem else pltpu.with_memory_space_constraint(a, pltpu.HBM if i in hbm else pltpu.VMEM)
        for i, a in enumerate(args)
    ))


def length_of(rows):
    return jnp.sqrt(jnp.sum(rows * rows, axis=1, keepdims=True) + EPS)


def text_body(raw_source, w_source, low_ref, raw_ref, w_ref, done):
    half = R // 2
    copies = [pltpu.make_async_copy(w_source, w_ref, done.at[2])]
    for i in range(2):
        rows = pl.ds(i * half, half)
        copies.append(pltpu.make_async_copy(raw_source.at[rows, :], raw_ref.at[rows, :], done.at[i]))
    for copy in copies:
        copy.start()
    for i in range(2):
        rows = pl.ds(i * half, half)
        copies[i + 1].wait()
        raw = raw_ref[rows, :].astype(F32)
        low_ref[rows, :] = (raw / length_of(raw)).astype(BF16)
    copies[0].wait()


def order_body(coord_ref, source_ref, pick_ref, xp_ref, xpt_ref, x_ref, done):
    copy = pltpu.make_async_copy(source_ref, x_ref, done)
    copy.start()
    y, z, x, c = (coord_ref[i] for i in range(4))
    row = lax.broadcasted_iota(jnp.int32, (SUB, 1), 0)
    within = (z + row // OWN + (NZ - 3)) % NZ * (NX * NC * OWN) + row % OWN
    lanes = lax.broadcasted_iota(jnp.int32, (SUB, D), 1)

    @pl.loop(0, D // COLS)
    def _(i):
        for j in range(COLS // SUB):
            group = i * (COLS // SUB) + j
            core = (c + group // 16) % NC
            second, first = group // 4 % 4, group % 4
            at_y = (y + jnp.where(core == 0, second, first)) % NY
            at_x = (x + jnp.where(core == 0, first, second)) % NX
            base = (at_y * (NZ * NX * NC) + at_x * NC + core) * OWN
            chosen = jnp.where(lanes == within + base, 1.0, 0.0).astype(BF16)
            pick_ref[pl.ds(pl.multiple_of(i * COLS + j * SUB, 16), SUB), :] = chosen

    copy.wait()

    @pl.loop(0, D // COLS)
    def _(i):
        rows = pl.ds(pl.multiple_of(i * COLS, COLS), COLS)
        xpt_ref[rows, :] = mm(pick_ref[rows, :], x_ref[...], NT).astype(BF16)
        xp_ref[:, rows] = mm(x_ref[...], pick_ref[rows, :], NT).astype(BF16)


def embed_body(xp_ref, *refs):
    pieces, (w_ref, unit_ref, low_ref, length_ref) = refs[:8], refs[8:]
    for i, piece in enumerate(pieces):
        w_ref[pl.ds(i * PIECE, PIECE), :] = piece[...]
    squares = jnp.zeros((R, 1), F32)
    for at in range(0, E, COLS):
        cols = pl.ds(at, COLS)
        part = mm(xp_ref[...], w_ref[:, cols])
        unit_ref[:, cols] = part
        squares = squares + jnp.sum(part * part, axis=1, keepdims=True)
    length = jnp.sqrt(squares + EPS)
    length_ref[...] = length
    unit = unit_ref[...] / length
    unit_ref[...] = unit
    low_ref[...] = unit.astype(BF16)


def derivative(rows, columns, scale, bias, diagonal):
    logits = scale * mm(rows, columns, NT) + bias
    if not diagonal:
        return (scale * jax.nn.sigmoid(logits)).astype(BF16)
    matched = lax.broadcasted_iota(jnp.int32, logits.shape, 0) == lax.broadcasted_iota(
        jnp.int32, logits.shape, 1
    )
    polarity = jnp.where(matched, 1.0, -1.0)
    return (-scale * polarity * jax.nn.sigmoid(-polarity * logits)).astype(BF16)


def image_body(scalar_ref, low_ref, unit_ref, length_ref, t0, t1, t2, t3, xpt_ref, eg_ref, s0, s1, s2, s3, grad, pair):
    scale, bias = scalar_ref[0], scalar_ref[1]
    texts = (t0, t1, t2, t3)
    for k, text in enumerate(texts):
        pair[k] = derivative(low_ref[...], text[...], scale, bias, k == 0)
    inner = jnp.zeros((R, 1), F32)
    for at in range(0, E, COLS):
        cols = pl.ds(at, COLS)
        part = mm(pair[0], t0[:, cols])
        for k in range(1, S):
            part = part + mm(pair[k], texts[k][:, cols])
        grad[:, cols] = part
        inner = inner + jnp.sum(part * unit_ref[:, cols], axis=1, keepdims=True)
    eg_ref[...] = ((grad[...] - unit_ref[...] * inner) / length_ref[...]).astype(BF16)
    for i, out in enumerate((s0, s1, s2, s3)):
        out[...] = mm(xpt_ref[pl.ds(HALF + i * PIECE, PIECE), :], eg_ref[...]).astype(BF16)


def weight_body(xpt_ref, eg_ref, came_ref, out, *, piece):
    rows = pl.ds(piece * PIECE, PIECE)
    out[...] = (mm(xpt_ref[rows, :], eg_ref[...]) + came_ref[...].astype(F32)).astype(BF16)


def join_body(*refs, rows):
    parts = [ref[...].astype(F32)[:n] for ref, n in zip(refs[:-1], rows, strict=True)]
    refs[-1][...] = jnp.concatenate(parts, 0).astype(BF16)


def stack_body(*refs):
    for i, ref in enumerate(refs[:-1]):
        refs[-1][pl.ds(i * SUB, SUB), :] = ref[...]


def features_body(eg_ref, w_ref, pick_ref, out_ref, mixed):
    @pl.loop(0, D // COLS)
    def _(i):
        rows = pl.ds(pl.multiple_of(i * COLS, COLS), COLS)
        mixed[:, rows] = mm(eg_ref[...], w_ref[rows, :], NT).astype(BF16)

    @pl.loop(0, D // COLS)
    def _(i):
        cols = pl.ds(pl.multiple_of(i * COLS, COLS), COLS)
        out_ref[:, cols] = mm(mixed[...], pick_ref[:, cols]).astype(BF16)


def text_grad_body(scalar_ref, raw_ref, low_ref, p0, p1, p2, p3, out_ref, grad, pair):
    scale, bias = scalar_ref[0], scalar_ref[1]
    images = (p0, p1, p2, p3)
    for k, image in enumerate(images):
        pair[k] = derivative(low_ref[...], image[...], scale, bias, k == 0)
    length = length_of(raw_ref[...].astype(F32))
    inner = jnp.zeros((R, 1), F32)
    for at in range(0, E, COLS):
        cols = pl.ds(at, COLS)
        part = mm(pair[0], p0[:, cols])
        for k in range(1, S):
            part = part + mm(pair[k], images[k][:, cols])
        grad[:, cols] = part
        inner = inner + jnp.sum(part * (raw_ref[:, cols].astype(F32) / length), axis=1, keepdims=True)
    out_ref[...] = ((grad[...] - raw_ref[...].astype(F32) / length * inner) / length).astype(BF16)


def sum_body(*refs, cuts):
    ins, outs = refs[:4], refs[4:]
    total = ins[0][...].astype(F32)
    for ref in ins[1:]:
        total = total + ref[...].astype(F32)
    for out, (lo, hi) in zip(outs, cuts, strict=True):
        out[...] = total[lo:hi].astype(BF16)


def near_body(mid_ref, low_ref, high_ref, *outs):
    mid, low, high = (ref[...].astype(F32) for ref in (mid_ref, low_ref, high_ref))
    outs[0][...] = (mid[:OWN] + low[:OWN] + high[:OWN]).astype(BF16)
    outs[1][...] = mid[OWN : 2 * OWN] + low[OWN:] + high[OWN : 2 * OWN]
    outs[2][...] = (mid[2 * OWN :] + high[2 * OWN :]).astype(BF16)


def join(rows, *parts):
    (out,) = call(functools.partial(join_body, rows=rows), [((sum(rows), E), BF16)], *parts, flops=10**6)
    return out


def gather_weight(kept, before, after):
    near = join((OWN,) * 3, before, kept, after)
    high, low = fetch(near, along_z(3)), fetch(near, along_z(-2))
    ring = join((2 * OWN, 3 * OWN, 3 * OWN), low, near, high)
    plane = [fetch(ring, along_first(d)) for d in (1, 2, 3)]
    (plane,) = call(stack_body, [((PIECE, E), BF16)], ring, *plane, flops=10**6)
    half = [plane] + [fetch(plane, along_second(d)) for d in (1, 2, 3)]
    return half + [fetch(piece, sibling) for piece in half]


def scatter_weight(pieces):
    got = [pieces[0]] + [fetch(pieces[d], along_second(-d)) for d in (1, 2, 3)]
    cuts = [(i * SUB, (i + 1) * SUB) for i in range(4)]
    pieces = call(functools.partial(sum_body, cuts=cuts), [((SUB, E), BF16)] * 4, *got, flops=10**8)
    got = [pieces[0]] + [fetch(pieces[d], along_first(-d)) for d in (1, 2, 3)]
    cuts = [(0, 2 * OWN), (2 * OWN, 5 * OWN), (5 * OWN, 8 * OWN)]
    low, mid, high = call(
        functools.partial(sum_body, cuts=cuts), [((hi - lo, E), BF16) for lo, hi in cuts], *got, flops=10**8
    )
    high, low = fetch(high, along_z(-3)), fetch(low, along_z(2))
    before, own, after = call(
        near_body, [((OWN, E), BF16), ((OWN, E), F32), ((OWN, E), BF16)], mid, low, high, flops=10**8
    )
    before, after = fetch(before, along_z(1)), fetch(after, along_z(-1))
    return own + before.astype(F32) + after.astype(F32)


def on_device(image_features, head_weight, text_embeds, natural_exponent_factor, logit_bias):
    scalars = jnp.concatenate([jnp.exp(natural_exponent_factor), logit_bias])
    place = jnp.stack([lax.axis_index(a) for a in AXES]).astype(jnp.int32)
    before = fetch(head_weight, along_z(-1))
    behind = fetch(head_weight, along_z(1))
    text_low, text_raw, kept = call(
        text_body, [((R, E), BF16), ((R, E), BF16), ((OWN, E), BF16)], text_embeds, head_weight,
        flops=10**8, hbm=(0, 1), scratch=[pltpu.SemaphoreType.DMA((3,))],
    )
    weight = gather_weight(kept, before, behind)
    texts = [text_low]
    for _ in range(1, S):
        texts.append(fetch(texts[-1], along_blocks(1)))
    pick, xp, xpt = call(
        order_body, [((D, D), BF16), ((R, D), BF16), ((D, R), BF16)], place, image_features,
        flops=4 * D * D * R, smem=(0,), hbm=(1,),
        scratch=[pltpu.VMEM((R, D), BF16), pltpu.SemaphoreType.DMA(())],
    )
    full, unit, low, length = call(
        embed_body, [((D, E), BF16), ((R, E), F32), ((R, E), BF16), ((R, 1), F32)], xp, *weight,
        flops=2 * R * D * E,
    )
    images = [low]
    for _ in range(1, S):
        images.append(fetch(images[-1], along_blocks(-1)))
    work = [pltpu.VMEM((R, E), F32), pltpu.VMEM((S, R, R), BF16)]
    eg, *sent = call(
        image_body, [((R, E), BF16)] + [((PIECE, E), BF16)] * 4, scalars, low, unit, length, *texts, xpt,
        flops=16 * R * R * E + 2 * R * HALF * E, scratch=work, smem=(0,),
    )
    came = [fetch(piece, sibling) for piece in sent]
    (grad_features,) = call(
        features_body, [((R, D), BF16)], eg, full, pick, flops=2 * R * D * E + 2 * R * D * D,
        scratch=[pltpu.VMEM((R, D), BF16)], final=True,
    )
    pieces = []
    for i in range(4):
        pieces += call(
            functools.partial(weight_body, piece=i), [((PIECE, E), BF16)], xpt, eg, came[i], flops=2 * R * PIECE * E
        )
    grad_weight = scatter_weight(pieces)
    (grad_text,) = call(
        text_grad_body, [((R, E), BF16)], scalars, text_raw, text_low, *images,
        flops=16 * R * R * E, scratch=work, smem=(0,), final=True,
    )
    return grad_features, grad_text, grad_weight


def solution(mesh):
    finer = Mesh(mesh.devices.reshape(NY, NZ, NX, NC), AXES)
    rows = P(AXES, None)

    return jax.shard_map(
        on_device,
        mesh=finer,
        in_specs=(rows, rows, rows, P(), P()),
        out_specs=(rows, rows, rows),
        check_vma=False,
    )
```

```python
import functools

import jax
import jax.numpy as jnp
from jax import lax
from jax.experimental import pallas as pl
from jax.experimental.pallas import tpu as pltpu
from jax.sharding import Mesh
from jax.sharding import PartitionSpec as P


S = 4
EPS = 1e-06
NY, NZ, NX, NC = 4, 8, 4, 2
NDEV = NY * NZ * NX * NC
AXES = ("y", "z", "x", "c")
R, D, E = 256, 1536, 1152
HALF = D // 2
PIECE = HALF // 4
SUB = PIECE // 4
OWN = D // NDEV
F32, BF16 = jnp.float32, jnp.bfloat16
NN = (((1,), (0,)), ((), ()))
NT = (((1,), (1,)), ((), ()))
COLS = 384


def mm(a, b, dims=NN):
    return lax.dot_general(a, b, dims, preferred_element_type=F32)


def index(y, z, x, c):
    return ((y % NY * NZ + z % NZ) * NX + x % NX) * NC + c % NC


def coords(i):
    return i // (NZ * NX * NC), i // (NX * NC) % NZ, i // NC % NX, i % NC


def fetch(value, where):
    return lax.ppermute(value, AXES, [(index(*where(*coords(i))), i) for i in range(NDEV)])


def along_z(d):
    return lambda y, z, x, c: (y, z + d, x, c)


def along_first(d):
    return lambda y, z, x, c: (y, z, x + d, c) if c == 0 else (y + d, z, x, c)


def along_second(d):
    return lambda y, z, x, c: (y + d, z, x, c) if c == 0 else (y, z, x + d, c)


def sibling(y, z, x, c):
    return y, z, x, 1 - c


def along_blocks(d):
    return lambda y, z, x, c: coords((index(y, z, x, c) + d) % NDEV)


def call(body, outs, *args, flops=0, scratch=(), smem=(), hbm=(), limit=8, final=False):
    def spec(i):
        return pl.BlockSpec(memory_space=pltpu.SMEM if i in smem else pltpu.HBM if i in hbm else pltpu.VMEM)

    return pl.pallas_call(
        body,
        out_shape=[jax.ShapeDtypeStruct(s, d) if final else pltpu.VMEM(s, d) for s, d in outs],
        in_specs=[spec(i) for i in range(len(args))],
        out_specs=[pl.BlockSpec(memory_space=pltpu.VMEM) for _ in outs],
        scratch_shapes=list(scratch),
        compiler_params=pltpu.CompilerParams(vmem_limit_bytes=limit << 20),
        cost_estimate=pl.CostEstimate(flops=flops, bytes_accessed=0, transcendentals=0),
    )(*(
        a if i in smem else pltpu.with_memory_space_constraint(a, pltpu.HBM if i in hbm else pltpu.VMEM)
        for i, a in enumerate(args)
    ))


def length_of(rows):
    return jnp.sqrt(jnp.sum(rows * rows, axis=1, keepdims=True) + EPS)


def text_body(raw_source, w_source, low_ref, raw_ref, w_ref, done):
    half = R // 2
    copies = [pltpu.make_async_copy(w_source, w_ref, done.at[2])]
    for i in range(2):
        rows = pl.ds(i * half, half)
        copies.append(pltpu.make_async_copy(raw_source.at[rows, :], raw_ref.at[rows, :], done.at[i]))
    for copy in copies:
        copy.start()
    for i in range(2):
        rows = pl.ds(i * half, half)
        copies[i + 1].wait()
        raw = raw_ref[rows, :].astype(F32)
        low_ref[rows, :] = (raw / length_of(raw)).astype(BF16)
    copies[0].wait()


def order_body(coord_ref, source_ref, pick_ref, xp_ref, xpt_ref, x_ref, done):
    copy = pltpu.make_async_copy(source_ref, x_ref, done)
    copy.start()
    y, z, x, c = (coord_ref[i] for i in range(4))
    row = lax.broadcasted_iota(jnp.int32, (SUB, 1), 0)
    within = (z + row // OWN + (NZ - 3)) % NZ * (NX * NC * OWN) + row % OWN
    lanes = lax.broadcasted_iota(jnp.int32, (SUB, D), 1)

    @pl.loop(0, D // COLS)
    def _(i):
        for j in range(COLS // SUB):
            group = i * (COLS // SUB) + j
            core = (c + group // 16) % NC
            second, first = group // 4 % 4, group % 4
            at_y = (y + jnp.where(core == 0, second, first)) % NY
            at_x = (x + jnp.where(core == 0, first, second)) % NX
            base = (at_y * (NZ * NX * NC) + at_x * NC + core) * OWN
            chosen = jnp.where(lanes == within + base, 1.0, 0.0).astype(BF16)
            pick_ref[pl.ds(pl.multiple_of(i * COLS + j * SUB, 16), SUB), :] = chosen

    copy.wait()

    @pl.loop(0, D // COLS)
    def _(i):
        rows = pl.ds(pl.multiple_of(i * COLS, COLS), COLS)
        xpt_ref[rows, :] = mm(pick_ref[rows, :], x_ref[...], NT).astype(BF16)
        xp_ref[:, rows] = mm(x_ref[...], pick_ref[rows, :], NT).astype(BF16)


def embed_body(xp_ref, *refs):
    pieces, (w_ref, unit_ref, low_ref, length_ref) = refs[:8], refs[8:]
    for i, piece in enumerate(pieces):
        w_ref[pl.ds(i * PIECE, PIECE), :] = piece[...]
    squares = jnp.zeros((R, 1), F32)
    for at in range(0, E, COLS):
        cols = pl.ds(at, COLS)
        part = mm(xp_ref[...], w_ref[:, cols])
        unit_ref[:, cols] = part
        squares = squares + jnp.sum(part * part, axis=1, keepdims=True)
    length = jnp.sqrt(squares + EPS)
    length_ref[...] = length
    unit = unit_ref[...] / length
    unit_ref[...] = unit
    low_ref[...] = unit.astype(BF16)


def derivative(rows, columns, scale, bias, diagonal):
    logits = scale * mm(rows, columns, NT) + bias
    if not diagonal:
        return (scale * jax.nn.sigmoid(logits)).astype(BF16)
    matched = lax.broadcasted_iota(jnp.int32, logits.shape, 0) == lax.broadcasted_iota(
        jnp.int32, logits.shape, 1
    )
    polarity = jnp.where(matched, 1.0, -1.0)
    return (-scale * polarity * jax.nn.sigmoid(-polarity * logits)).astype(BF16)


def image_body(scalar_ref, low_ref, unit_ref, length_ref, t0, t1, t2, t3, eg_ref, grad, pair):
    scale, bias = scalar_ref[0], scalar_ref[1]
    texts = (t0, t1, t2, t3)
    for k, text in enumerate(texts):
        pair[k] = derivative(low_ref[...], text[...], scale, bias, k == 0)
    inner = jnp.zeros((R, 1), F32)
    for at in range(0, E, COLS):
        cols = pl.ds(at, COLS)
        part = mm(pair[0], t0[:, cols])
        for k in range(1, S):
            part = part + mm(pair[k], texts[k][:, cols])
        grad[:, cols] = part
        inner = inner + jnp.sum(part * unit_ref[:, cols], axis=1, keepdims=True)
    eg_ref[...] = ((grad[...] - unit_ref[...] * inner) / length_ref[...]).astype(BF16)


def sibling_body(xpt_ref, eg_ref, out, *, piece):
    out[...] = mm(xpt_ref[pl.ds(HALF + piece * PIECE, PIECE), :], eg_ref[...]).astype(BF16)


def weight_body(xpt_ref, eg_ref, came_ref, out, *, piece):
    rows = pl.ds(piece * PIECE, PIECE)
    out[...] = (mm(xpt_ref[rows, :], eg_ref[...]) + came_ref[...].astype(F32)).astype(BF16)


def join_body(*refs, rows):
    parts = [ref[...].astype(F32)[:n] for ref, n in zip(refs[:-1], rows, strict=True)]
    refs[-1][...] = jnp.concatenate(parts, 0).astype(BF16)


def stack_body(*refs):
    for i, ref in enumerate(refs[:-1]):
        refs[-1][pl.ds(i * SUB, SUB), :] = ref[...]


def features_body(eg_ref, w_ref, pick_ref, out_ref, mixed):
    @pl.loop(0, D // COLS)
    def _(i):
        rows = pl.ds(pl.multiple_of(i * COLS, COLS), COLS)
        mixed[:, rows] = mm(eg_ref[...], w_ref[rows, :], NT).astype(BF16)

    @pl.loop(0, D // COLS)
    def _(i):
        cols = pl.ds(pl.multiple_of(i * COLS, COLS), COLS)
        out_ref[:, cols] = mm(mixed[...], pick_ref[:, cols]).astype(BF16)


def text_part_body(scalar_ref, low_ref, p0, p1, p2, grad_ref, pair):
    scale, bias = scalar_ref[0], scalar_ref[1]
    images = (p0, p1, p2)
    for k, image in enumerate(images):
        pair[k] = derivative(low_ref[...], image[...], scale, bias, k == 0)
    for at in range(0, E, COLS):
        cols = pl.ds(at, COLS)
        part = mm(pair[0], p0[:, cols])
        for k in range(1, S - 1):
            part = part + mm(pair[k], images[k][:, cols])
        grad_ref[:, cols] = part


def text_grad_body(scalar_ref, raw_ref, low_ref, p3, part_ref, out_ref, grad):
    scale, bias = scalar_ref[0], scalar_ref[1]
    pair = derivative(low_ref[...], p3[...], scale, bias, False)
    length = length_of(raw_ref[...].astype(F32))
    inner = jnp.zeros((R, 1), F32)
    for at in range(0, E, COLS):
        cols = pl.ds(at, COLS)
        part = part_ref[:, cols] + mm(pair, p3[:, cols])
        grad[:, cols] = part
        inner = inner + jnp.sum(part * (raw_ref[:, cols].astype(F32) / length), axis=1, keepdims=True)
    out_ref[...] = ((grad[...] - raw_ref[...].astype(F32) / length * inner) / length).astype(BF16)


def sum_body(*refs, cuts):
    ins, outs = refs[:4], refs[4:]
    total = ins[0][...].astype(F32)
    for ref in ins[1:]:
        total = total + ref[...].astype(F32)
    for out, (lo, hi) in zip(outs, cuts, strict=True):
        out[...] = total[lo:hi].astype(BF16)


def near_body(mid_ref, low_ref, high_ref, *outs):
    mid, low, high = (ref[...].astype(F32) for ref in (mid_ref, low_ref, high_ref))
    outs[0][...] = (mid[:OWN] + low[:OWN] + high[:OWN]).astype(BF16)
    outs[1][...] = mid[OWN : 2 * OWN] + low[OWN:] + high[OWN : 2 * OWN]
    outs[2][...] = (mid[2 * OWN :] + high[2 * OWN :]).astype(BF16)


def join(rows, *parts):
    (out,) = call(functools.partial(join_body, rows=rows), [((sum(rows), E), BF16)], *parts, flops=10**6)
    return out


def gather_weight(kept, before, after):
    near = join((OWN,) * 3, before, kept, after)
    high, low = fetch(near, along_z(3)), fetch(near, along_z(-2))
    ring = join((2 * OWN, 3 * OWN, 3 * OWN), low, near, high)
    plane = [fetch(ring, along_first(d)) for d in (1, 2, 3)]
    (plane,) = call(stack_body, [((PIECE, E), BF16)], ring, *plane, flops=10**6)
    half = [plane] + [fetch(plane, along_second(d)) for d in (1, 2, 3)]
    return half + [fetch(piece, sibling) for piece in half]


def scatter_weight(pieces):
    got = [pieces[0]] + [fetch(pieces[d], along_second(-d)) for d in (1, 2, 3)]
    cuts = [(i * SUB, (i + 1) * SUB) for i in range(4)]
    pieces = call(functools.partial(sum_body, cuts=cuts), [((SUB, E), BF16)] * 4, *got, flops=10**8)
    got = [pieces[0]] + [fetch(pieces[d], along_first(-d)) for d in (1, 2, 3)]
    cuts = [(0, 2 * OWN), (2 * OWN, 5 * OWN), (5 * OWN, 8 * OWN)]
    low, mid, high = call(
        functools.partial(sum_body, cuts=cuts), [((hi - lo, E), BF16) for lo, hi in cuts], *got, flops=10**8
    )
    high, low = fetch(high, along_z(-3)), fetch(low, along_z(2))
    before, own, after = call(
        near_body, [((OWN, E), BF16), ((OWN, E), F32), ((OWN, E), BF16)], mid, low, high, flops=10**8
    )
    before, after = fetch(before, along_z(1)), fetch(after, along_z(-1))
    return own + before.astype(F32) + after.astype(F32)


def on_device(image_features, head_weight, text_embeds, natural_exponent_factor, logit_bias):
    scalars = jnp.concatenate([jnp.exp(natural_exponent_factor), logit_bias])
    place = jnp.stack([lax.axis_index(a) for a in AXES]).astype(jnp.int32)
    before = fetch(head_weight, along_z(-1))
    behind = fetch(head_weight, along_z(1))
    text_low, text_raw, kept = call(
        text_body, [((R, E), BF16), ((R, E), BF16), ((OWN, E), BF16)], text_embeds, head_weight,
        flops=10**8, hbm=(0, 1), scratch=[pltpu.SemaphoreType.DMA((3,))],
    )
    weight = gather_weight(kept, before, behind)
    texts = [text_low]
    for _ in range(1, S):
        texts.append(fetch(texts[-1], along_blocks(1)))
    pick, xp, xpt = call(
        order_body, [((D, D), BF16), ((R, D), BF16), ((D, R), BF16)], place, image_features,
        flops=4 * D * D * R, smem=(0,), hbm=(1,),
        scratch=[pltpu.VMEM((R, D), BF16), pltpu.SemaphoreType.DMA(())],
    )
    full, unit, low, length = call(
        embed_body, [((D, E), BF16), ((R, E), F32), ((R, E), BF16), ((R, 1), F32)], xp, *weight,
        flops=2 * R * D * E,
    )
    images = [low]
    for _ in range(1, S):
        images.append(fetch(images[-1], along_blocks(-1)))
    work = [pltpu.VMEM((R, E), F32), pltpu.VMEM((S, R, R), BF16)]
    (eg,) = call(
        image_body, [((R, E), BF16)], scalars, low, unit, length, *texts,
        flops=16 * R * R * E, scratch=work, smem=(0,),
    )
    came = []
    for i in range(4):
        (sent,) = call(functools.partial(sibling_body, piece=i), [((PIECE, E), BF16)], xpt, eg, flops=2 * R * PIECE * E)
        came.append(fetch(sent, sibling))
    (grad_features,) = call(
        features_body, [((R, D), BF16)], eg, full, pick, flops=2 * R * D * E + 2 * R * D * D,
        scratch=[pltpu.VMEM((R, D), BF16)], final=True,
    )
    pieces = []
    for i in range(4):
        pieces += call(
            functools.partial(weight_body, piece=i), [((PIECE, E), BF16)], xpt, eg, came[i], flops=2 * R * PIECE * E
        )
    grad_weight = scatter_weight(pieces)
    (part,) = call(
        text_part_body, [((R, E), F32)], scalars, text_low, *images[:3],
        flops=12 * R * R * E, scratch=[pltpu.VMEM((S - 1, R, R), BF16)], smem=(0,),
    )
    (grad_text,) = call(
        text_grad_body, [((R, E), BF16)], scalars, text_raw, text_low, images[3], part,
        flops=4 * R * R * E, scratch=work[:1], smem=(0,), final=True,
    )
    return grad_features, grad_text, grad_weight


def solution(mesh):
    finer = Mesh(mesh.devices.reshape(NY, NZ, NX, NC), AXES)
    rows = P(AXES, None)

    return jax.shard_map(
        on_device,
        mesh=finer,
        in_specs=(rows, rows, rows, P(), P()),
        out_specs=(rows, rows, rows),
        check_vma=False,
    )
```

```python
import functools

import jax
import jax.numpy as jnp
from jax import lax
from jax.experimental import pallas as pl
from jax.experimental.pallas import tpu as pltpu
from jax.sharding import Mesh
from jax.sharding import PartitionSpec as P


S = 4
EPS = 1e-06
NY, NZ, NX, NC = 4, 8, 4, 2
NDEV = NY * NZ * NX * NC
AXES = ("y", "z", "x", "c")
R, D, E = 256, 1536, 1152
HALF = D // 2
PIECE = HALF // 4
SUB = PIECE // 4
OWN = D // NDEV
F32, BF16 = jnp.float32, jnp.bfloat16
NN = (((1,), (0,)), ((), ()))
NT = (((1,), (1,)), ((), ()))
COLS = 384


def mm(a, b, dims=NN):
    return lax.dot_general(a, b, dims, preferred_element_type=F32)


def index(y, z, x, c):
    return ((y % NY * NZ + z % NZ) * NX + x % NX) * NC + c % NC


def coords(i):
    return i // (NZ * NX * NC), i // (NX * NC) % NZ, i // NC % NX, i % NC


def fetch(value, where):
    return lax.ppermute(value, AXES, [(index(*where(*coords(i))), i) for i in range(NDEV)])


def along_z(d):
    return lambda y, z, x, c: (y, z + d, x, c)


def along_first(d):
    return lambda y, z, x, c: (y, z, x + d, c) if c == 0 else (y + d, z, x, c)


def along_second(d):
    return lambda y, z, x, c: (y + d, z, x, c) if c == 0 else (y, z, x + d, c)


def sibling(y, z, x, c):
    return y, z, x, 1 - c


def along_blocks(d):
    return lambda y, z, x, c: coords((index(y, z, x, c) + d) % NDEV)


def call(body, outs, *args, flops=0, scratch=(), smem=(), hbm=(), limit=8, final=False):
    def spec(i):
        return pl.BlockSpec(memory_space=pltpu.SMEM if i in smem else pltpu.HBM if i in hbm else pltpu.VMEM)

    return pl.pallas_call(
        body,
        out_shape=[jax.ShapeDtypeStruct(s, d) if final else pltpu.VMEM(s, d) for s, d in outs],
        in_specs=[spec(i) for i in range(len(args))],
        out_specs=[pl.BlockSpec(memory_space=pltpu.VMEM) for _ in outs],
        scratch_shapes=list(scratch),
        compiler_params=pltpu.CompilerParams(vmem_limit_bytes=limit << 20),
        cost_estimate=pl.CostEstimate(flops=flops, bytes_accessed=0, transcendentals=0),
    )(*(
        a if i in smem else pltpu.with_memory_space_constraint(a, pltpu.HBM if i in hbm else pltpu.VMEM)
        for i, a in enumerate(args)
    ))


def length_of(rows):
    return jnp.sqrt(jnp.sum(rows * rows, axis=1, keepdims=True) + EPS)


def text_body(raw_source, w_source, low_ref, raw_ref, w_ref, done):
    half = R // 2
    copies = [pltpu.make_async_copy(w_source, w_ref, done.at[2])]
    for i in range(2):
        rows = pl.ds(i * half, half)
        copies.append(pltpu.make_async_copy(raw_source.at[rows, :], raw_ref.at[rows, :], done.at[i]))
    for copy in copies:
        copy.start()
    for i in range(2):
        rows = pl.ds(i * half, half)
        copies[i + 1].wait()
        raw = raw_ref[rows, :].astype(F32)
        low_ref[rows, :] = (raw / length_of(raw)).astype(BF16)
    copies[0].wait()


def order_body(coord_ref, source_ref, pick_ref, xp_ref, xpt_ref, x_ref, done):
    copy = pltpu.make_async_copy(source_ref, x_ref, done)
    copy.start()
    y, z, x, c = (coord_ref[i] for i in range(4))
    row = lax.broadcasted_iota(jnp.int32, (SUB, 1), 0)
    within = (z + row // OWN + (NZ - 4)) % NZ * (NX * NC * OWN) + row % OWN
    lanes = lax.broadcasted_iota(jnp.int32, (SUB, D), 1)

    @pl.loop(0, D // COLS)
    def _(i):
        for j in range(COLS // SUB):
            group = i * (COLS // SUB) + j
            core = (c + group // 16) % NC
            second, first = group // 4 % 4, group % 4
            at_y = (y + jnp.where(core == 0, second, first)) % NY
            at_x = (x + jnp.where(core == 0, first, second)) % NX
            base = (at_y * (NZ * NX * NC) + at_x * NC + core) * OWN
            chosen = jnp.where(lanes == within + base, 1.0, 0.0).astype(BF16)
            pick_ref[pl.ds(pl.multiple_of(i * COLS + j * SUB, 16), SUB), :] = chosen

    copy.wait()

    @pl.loop(0, D // COLS)
    def _(i):
        rows = pl.ds(pl.multiple_of(i * COLS, COLS), COLS)
        xpt_ref[rows, :] = mm(pick_ref[rows, :], x_ref[...], NT).astype(BF16)
        xp_ref[:, rows] = mm(x_ref[...], pick_ref[rows, :], NT).astype(BF16)


def stacked(pieces, w_ref):
    for i, piece in enumerate(pieces):
        w_ref[pl.ds(i * PIECE, PIECE), :] = piece[...]


def embed_part_body(xp_ref, *refs):
    pieces, (w_ref, part_ref) = refs[:4], refs[4:]
    stacked(pieces, w_ref)
    for at in range(0, E, COLS):
        cols = pl.ds(at, COLS)
        part_ref[:, cols] = mm(xp_ref[:, pl.ds(0, HALF)], w_ref[:, cols])


def embed_body(xp_ref, part_ref, *refs):
    pieces, (w_ref, unit_ref, low_ref, length_ref) = refs[:4], refs[4:]
    stacked(pieces, w_ref)
    squares = jnp.zeros((R, 1), F32)
    for at in range(0, E, COLS):
        cols = pl.ds(at, COLS)
        part = part_ref[:, cols] + mm(xp_ref[:, pl.ds(HALF, HALF)], w_ref[:, cols])
        unit_ref[:, cols] = part
        squares = squares + jnp.sum(part * part, axis=1, keepdims=True)
    length = jnp.sqrt(squares + EPS)
    length_ref[...] = length
    unit = unit_ref[...] / length
    unit_ref[...] = unit
    low_ref[...] = unit.astype(BF16)


def derivative(rows, columns, scale, bias, diagonal):
    logits = scale * mm(rows, columns, NT) + bias
    if not diagonal:
        return (scale * jax.nn.sigmoid(logits)).astype(BF16)
    matched = lax.broadcasted_iota(jnp.int32, logits.shape, 0) == lax.broadcasted_iota(
        jnp.int32, logits.shape, 1
    )
    polarity = jnp.where(matched, 1.0, -1.0)
    return (-scale * polarity * jax.nn.sigmoid(-polarity * logits)).astype(BF16)


def image_body(scalar_ref, low_ref, unit_ref, length_ref, t0, t1, t2, t3, eg_ref, grad, pair):
    scale, bias = scalar_ref[0], scalar_ref[1]
    texts = (t0, t1, t2, t3)
    for k, text in enumerate(texts):
        pair[k] = derivative(low_ref[...], text[...], scale, bias, k == 0)
    inner = jnp.zeros((R, 1), F32)
    for at in range(0, E, COLS):
        cols = pl.ds(at, COLS)
        part = mm(pair[0], t0[:, cols])
        for k in range(1, S):
            part = part + mm(pair[k], texts[k][:, cols])
        grad[:, cols] = part
        inner = inner + jnp.sum(part * unit_ref[:, cols], axis=1, keepdims=True)
    eg_ref[...] = ((grad[...] - unit_ref[...] * inner) / length_ref[...]).astype(BF16)


def sibling_body(xpt_ref, eg_ref, out, *, piece):
    out[...] = mm(xpt_ref[pl.ds(HALF + piece * PIECE, PIECE), :], eg_ref[...]).astype(BF16)


def weight_body(xpt_ref, eg_ref, came_ref, out, *, piece):
    rows = pl.ds(piece * PIECE, PIECE)
    out[...] = (mm(xpt_ref[rows, :], eg_ref[...]) + came_ref[...].astype(F32)).astype(BF16)


def join_body(*refs, rows):
    parts = [ref[...].astype(F32)[:n] for ref, n in zip(refs[:-1], rows, strict=True)]
    refs[-1][...] = jnp.concatenate(parts, 0).astype(BF16)


def stack_body(*refs):
    for i, ref in enumerate(refs[:-1]):
        refs[-1][pl.ds(i * SUB, SUB), :] = ref[...]


def features_body(eg_ref, own_ref, other_ref, pick_ref, out_ref, mixed):
    for half, w_ref in enumerate((own_ref, other_ref)):
        for at in range(0, HALF, COLS):
            part = mm(eg_ref[...], w_ref[pl.ds(at, COLS), :], NT)
            mixed[:, pl.ds(half * HALF + at, COLS)] = part.astype(BF16)

    @pl.loop(0, D // COLS)
    def _(i):
        cols = pl.ds(pl.multiple_of(i * COLS, COLS), COLS)
        out_ref[:, cols] = mm(mixed[...], pick_ref[:, cols]).astype(BF16)


def text_part_body(scalar_ref, low_ref, p0, p1, p2, grad_ref, pair):
    scale, bias = scalar_ref[0], scalar_ref[1]
    images = (p0, p1, p2)
    for k, image in enumerate(images):
        pair[k] = derivative(low_ref[...], image[...], scale, bias, k == 0)
    for at in range(0, E, COLS):
        cols = pl.ds(at, COLS)
        part = mm(pair[0], p0[:, cols])
        for k in range(1, S - 1):
            part = part + mm(pair[k], images[k][:, cols])
        grad_ref[:, cols] = part


def text_grad_body(scalar_ref, raw_ref, low_ref, p3, part_ref, out_ref, grad):
    scale, bias = scalar_ref[0], scalar_ref[1]
    pair = derivative(low_ref[...], p3[...], scale, bias, False)
    length = length_of(raw_ref[...].astype(F32))
    inner = jnp.zeros((R, 1), F32)
    for at in range(0, E, COLS):
        cols = pl.ds(at, COLS)
        part = part_ref[:, cols] + mm(pair, p3[:, cols])
        grad[:, cols] = part
        inner = inner + jnp.sum(part * (raw_ref[:, cols].astype(F32) / length), axis=1, keepdims=True)
    out_ref[...] = ((grad[...] - raw_ref[...].astype(F32) / length * inner) / length).astype(BF16)


def sum_body(*refs, cuts):
    ins, outs = refs[:4], refs[4:]
    total = ins[0][...].astype(F32)
    for ref in ins[1:]:
        total = total + ref[...].astype(F32)
    for out, (lo, hi) in zip(outs, cuts, strict=True):
        out[...] = total[lo:hi].astype(BF16)


def near_body(mid_ref, low_ref, high_ref, *outs):
    mid, low, high = (ref[...].astype(F32) for ref in (mid_ref, low_ref, high_ref))
    outs[0][...] = (mid[:OWN] + low[:OWN]).astype(BF16)
    outs[1][...] = mid[OWN : 2 * OWN] + low[OWN : 2 * OWN] + high[:OWN]
    outs[2][...] = (mid[2 * OWN :] + low[2 * OWN :] + high[OWN:]).astype(BF16)


def join(rows, *parts):
    (out,) = call(functools.partial(join_body, rows=rows), [((sum(rows), E), BF16)], *parts, flops=10**6)
    return out


def gather_weight(kept, before, after):
    near = join((OWN,) * 3, before, kept, after)
    near_high = join((OWN,) * 2, kept, after)
    low, high = fetch(near, along_z(-3)), fetch(near_high, along_z(2))
    ring = join((3 * OWN, 3 * OWN, 2 * OWN), low, near, high)
    plane = [fetch(ring, along_first(d)) for d in (1, 2, 3)]
    (plane,) = call(stack_body, [((PIECE, E), BF16)], ring, *plane, flops=10**6)
    half = [plane] + [fetch(plane, along_second(d)) for d in (1, 2, 3)]
    return half + [fetch(piece, sibling) for piece in half]


def scatter_weight(pieces):
    got = [pieces[0]] + [fetch(pieces[d], along_second(-d)) for d in (1, 2, 3)]
    cuts = [(i * SUB, (i + 1) * SUB) for i in range(4)]
    pieces = call(functools.partial(sum_body, cuts=cuts), [((SUB, E), BF16)] * 4, *got, flops=10**8)
    got = [pieces[0]] + [fetch(pieces[d], along_first(-d)) for d in (1, 2, 3)]
    cuts = [(0, 3 * OWN), (3 * OWN, 6 * OWN), (6 * OWN, 8 * OWN)]
    low, mid, high = call(
        functools.partial(sum_body, cuts=cuts), [((hi - lo, E), BF16) for lo, hi in cuts], *got, flops=10**8
    )
    low, high = fetch(low, along_z(3)), fetch(high, along_z(-2))
    before, own, after = call(
        near_body, [((OWN, E), BF16), ((OWN, E), F32), ((OWN, E), BF16)], mid, low, high, flops=10**8
    )
    before, after = fetch(before, along_z(1)), fetch(after, along_z(-1))
    return own + before.astype(F32) + after.astype(F32)


def on_device(image_features, head_weight, text_embeds, natural_exponent_factor, logit_bias):
    scalars = jnp.concatenate([jnp.exp(natural_exponent_factor), logit_bias])
    place = jnp.stack([lax.axis_index(a) for a in AXES]).astype(jnp.int32)
    before = fetch(head_weight, along_z(-1))
    behind = fetch(head_weight, along_z(1))
    text_low, text_raw, kept = call(
        text_body, [((R, E), BF16), ((R, E), BF16), ((OWN, E), BF16)], text_embeds, head_weight,
        flops=10**8, hbm=(0, 1), scratch=[pltpu.SemaphoreType.DMA((3,))],
    )
    weight = gather_weight(kept, before, behind)
    texts = [text_low]
    for _ in range(1, S):
        texts.append(fetch(texts[-1], along_blocks(1)))
    pick, xp, xpt = call(
        order_body, [((D, D), BF16), ((R, D), BF16), ((D, R), BF16)], place, image_features,
        flops=4 * D * D * R, smem=(0,), hbm=(1,),
        scratch=[pltpu.VMEM((R, D), BF16), pltpu.SemaphoreType.DMA(())],
    )
    own_rows, part = call(embed_part_body, [((HALF, E), BF16), ((R, E), F32)], xp, *weight[:4], flops=2 * R * HALF * E)
    other_rows, unit, low, length = call(
        embed_body, [((HALF, E), BF16), ((R, E), F32), ((R, E), BF16), ((R, 1), F32)], xp, part, *weight[4:],
        flops=2 * R * HALF * E,
    )
    images = [low]
    for _ in range(1, S):
        images.append(fetch(images[-1], along_blocks(-1)))
    work = [pltpu.VMEM((R, E), F32), pltpu.VMEM((S, R, R), BF16)]
    (eg,) = call(
        image_body, [((R, E), BF16)], scalars, low, unit, length, *texts,
        flops=16 * R * R * E, scratch=work, smem=(0,),
    )
    came = []
    for i in range(4):
        (sent,) = call(functools.partial(sibling_body, piece=i), [((PIECE, E), BF16)], xpt, eg, flops=2 * R * PIECE * E)
        came.append(fetch(sent, sibling))
    (grad_features,) = call(
        features_body, [((R, D), BF16)], eg, own_rows, other_rows, pick, flops=2 * R * D * E + 2 * R * D * D,
        scratch=[pltpu.VMEM((R, D), BF16)], final=True,
    )
    pieces = []
    for i in range(4):
        pieces += call(
            functools.partial(weight_body, piece=i), [((PIECE, E), BF16)], xpt, eg, came[i], flops=2 * R * PIECE * E
        )
    grad_weight = scatter_weight(pieces)
    (part,) = call(
        text_part_body, [((R, E), F32)], scalars, text_low, *images[:3],
        flops=12 * R * R * E, scratch=[pltpu.VMEM((S - 1, R, R), BF16)], smem=(0,),
    )
    (grad_text,) = call(
        text_grad_body, [((R, E), BF16)], scalars, text_raw, text_low, images[3], part,
        flops=4 * R * R * E, scratch=work[:1], smem=(0,), final=True,
    )
    return grad_features, grad_text, grad_weight


def solution(mesh):
    finer = Mesh(mesh.devices.reshape(NY, NZ, NX, NC), AXES)
    rows = P(AXES, None)

    return jax.shard_map(
        on_device,
        mesh=finer,
        in_specs=(rows, rows, rows, P(), P()),
        out_specs=(rows, rows, rows),
        check_vma=False,
    )
```
